128 devices in a mesh: seq: 16 (over z_lo, y, core), head: 8 (over x, z_hi).
Axes of the slice: x: 4, y: 4, z: 4 (z_hi: 2, z_lo: 2; z = z_hi * 2 + z_lo), core: 2. Of those that a mesh axis runs over, the one named last changes fastest.
Arguments:
- queries: bfloat16 [16, 128, 8192], P('seq', None, 'head'), may hold values from -160 to 160
- continuation_key_slots: bfloat16 [16, 128, 1024], P('seq', None, 'head'), may hold values from -13.1875 to 13.1875
- continuation_value_slots: bfloat16 [16, 128, 1024], P('seq', None, 'head'), may hold values from -24 to 24
- cached_prompt_keys: bfloat16 [2, 16384, 1024], P(None, 'seq', 'head'), may hold values from -6 to 6
- cached_prompt_values: bfloat16 [2, 16384, 1024], P(None, 'seq', 'head'), may hold values from -24 to 24
- pair_lengths: int32 [4, 2], replicated, may hold values from 1 to 256
- prompt_of: int32 [4], replicated, may hold values from 0 to 1
- slot_tile: int32 [16], replicated, may hold values from 0 to 15, each once
- out_weight: bfloat16 [8192, 8192], P('head', 'seq'), may hold values from -0.0625 to 0.0625
Outputs:
- projected: bfloat16 [16, 128, 8192], P('head', None, 'seq')
The draws below stay inside these ranges and needn't reach their ends.
Inputs may be any that keep to these rules, and one draw needn't show every extreme that they name: `slot_tile`: each of the 16 tiles stands in exactly one slot.
All inputs are finite; a program needn't handle non-finite values.
Results may differ from the reference program's by a relative error of at most 0.014.
Values may be sent and summed in bfloat16 or wider, within the bound.
A program may use at most 128 MiB of HBM per device.

```python
import math
from functools import partial
import jax
import jax.numpy as jnp
from jax import lax

D = 8192
QUERY_HEADS = 64
KEY_VALUE_HEADS = 8
HEAD_WIDTH = 128
TILE_ROWS = 128
MAX_CONT_TILES = 2
PROMPT_COUNT = 2
TILE_SLOTS = 16
PAIRS = 4
PROMPT_LENGTH = 16384


def prompt_key_block(key):
    sampled_keys = jax.random.truncated_normal(jax.random.fold_in(key, 101), -6.0, 6.0, (PROMPT_COUNT, PROMPT_LENGTH, KEY_VALUE_HEADS * HEAD_WIDTH), jnp.float32)
    return sampled_keys


def draw_cached_prompt_keys(key, part):
    return prompt_key_block(key).astype(jnp.bfloat16)


def draw_queries(key, part):
    drawn = 2.5 * jax.random.truncated_normal(jax.random.fold_in(key, 202), -6.0, 6.0, (TILE_SLOTS, TILE_ROWS, QUERY_HEADS * HEAD_WIDTH), jnp.float32)
    return drawn.astype(jnp.bfloat16)


def plant(values, key, smallest, largest):
    longest = values.shape.index(max(values.shape))
    spots = []
    for shift in (0, 1):
        where = [jax.random.randint(jax.random.fold_in(key, axis), (), 0, length) for axis, length in enumerate(values.shape)]
        where[longest] = (where[longest] + shift) % values.shape[longest]
        spots.append(tuple(where))
    return values.at[spots[0]].set(smallest).at[spots[1]].set(largest)


def levels(rng, extent, cuts, least, largest):
    def one(position, shards_of):
        heights = jax.random.uniform(jax.random.fold_in(jax.random.fold_in(rng, 6), position), (shards_of,), jnp.float32, least / len(cuts), largest / len(cuts))
        return jnp.repeat(jnp.exp(heights), extent[position] // shards_of).reshape((-1,) + (1,) * (len(extent) - position - 1))

    factor_of = one(*cuts[0])
    for cut in cuts[1:]:
        factor_of = factor_of * one(*cut)
    return factor_of


def noise(rng, shape, spread, limit, shards=(), kind=jnp.bfloat16):
    result = spread * jax.random.normal(rng, shape, jnp.float32)
    if shards:
        result = result * levels(rng, shape, shards, -0.22, 0.18)
    return jnp.clip(result, -limit, limit).astype(kind)


def setup_inputs(seed: int = 0) -> dict:
    splits = jax.random.split(jax.random.key(seed), 10)
    queries = draw_queries(jax.random.fold_in(splits[9], 71), 0)
    continuation_key_slots = noise(splits[1], (TILE_SLOTS, TILE_ROWS, KEY_VALUE_HEADS * HEAD_WIDTH), 2.2, 13.1875, ((0, 16), (2, 8)))
    continuation_value_slots = noise(splits[2], (TILE_SLOTS, TILE_ROWS, KEY_VALUE_HEADS * HEAD_WIDTH), 4.0, 24.0, ((0, 16), (2, 8)))
    cached_prompt_keys = draw_cached_prompt_keys(jax.random.fold_in(splits[9], 71), 0)
    cached_prompt_values = noise(splits[4], (PROMPT_COUNT, PROMPT_LENGTH, KEY_VALUE_HEADS * HEAD_WIDTH), 4.0, 24.0, ((1, 16), (2, 8)))
    pair_lengths = plant(jax.random.randint(splits[5], (PAIRS, 2), 1, MAX_CONT_TILES * TILE_ROWS + 1), jax.random.fold_in(splits[5], 1), 1, MAX_CONT_TILES * TILE_ROWS).astype(jnp.int32)
    prompt_of = plant(jax.random.randint(splits[6], (PAIRS,), 0, PROMPT_COUNT), jax.random.fold_in(splits[6], 1), 0, PROMPT_COUNT - 1).astype(jnp.int32)
    slot_tile = jax.random.permutation(splits[7], TILE_SLOTS).astype(jnp.int32)
    out_weight = noise(splits[8], (QUERY_HEADS * HEAD_WIDTH, D), (QUERY_HEADS * HEAD_WIDTH) ** -0.5, 0.0625, ((0, 8), (1, 16)))
    return {"queries": queries, "continuation_key_slots": continuation_key_slots, "continuation_value_slots": continuation_value_slots, "cached_prompt_keys": cached_prompt_keys, "cached_prompt_values": cached_prompt_values, "pair_lengths": pair_lengths, "prompt_of": prompt_of, "slot_tile": slot_tile, "out_weight": out_weight}


VERY_LOW = -1e+30

def round_weights(weights):
    rounded = lax.optimization_barrier(weights.astype(jnp.bfloat16))
    return rounded.astype(jnp.float32)

def group_attention(items, causal, scaling):
    query_group, prompt_key_rows, prompt_value_rows, self_key_block, self_value_block = items
    prompt_scores = jnp.einsum('tgd,pd->gtp', query_group, prompt_key_rows, precision=lax.Precision.HIGHEST) * scaling
    own_scores = jnp.einsum('tgd,pd->gtp', query_group, self_key_block, precision=lax.Precision.HIGHEST) * scaling
    own_scores = jnp.where(causal[None], own_scores, VERY_LOW)
    peak = jnp.maximum(lax.optimization_barrier(jnp.max(prompt_scores, axis=2)), lax.optimization_barrier(jnp.max(own_scores, axis=2)))
    prompt_w = jnp.exp(prompt_scores - peak[:, :, None])
    own_w = jnp.exp(own_scores - peak[:, :, None])
    denominator = lax.optimization_barrier(jnp.sum(prompt_w, axis=2)) + lax.optimization_barrier(jnp.sum(own_w, axis=2))
    numerator = jnp.einsum('gtp,pd->gtd', round_weights(prompt_w), prompt_value_rows, precision=lax.Precision.HIGHEST)
    numerator = numerator + jnp.einsum('gtp,pd->gtd', round_weights(own_w), self_value_block, precision=lax.Precision.HIGHEST)
    return numerator / denominator[:, :, None]

def reference(queries, continuation_key_slots, continuation_value_slots, cached_prompt_keys, cached_prompt_values, pair_lengths, prompt_of, slot_tile, out_weight):
    scaling = 1.0 / math.sqrt(HEAD_WIDTH)
    owner_slot = jnp.zeros((TILE_SLOTS,), jnp.int32).at[slot_tile].set(jnp.arange(TILE_SLOTS, dtype=jnp.int32))
    lengths = pair_lengths.reshape(2 * PAIRS)

    def one_slot(slot_index):
        tile_id = slot_tile[slot_index]
        continuation = tile_id // MAX_CONT_TILES
        offset = tile_id % MAX_CONT_TILES * TILE_ROWS
        prompt_index = prompt_of[continuation // 2]
        prompt_key_rows = lax.dynamic_index_in_dim(cached_prompt_keys, prompt_index, 0, False).astype(jnp.float32).reshape(PROMPT_LENGTH, KEY_VALUE_HEADS, HEAD_WIDTH)
        prompt_value_rows = lax.dynamic_index_in_dim(cached_prompt_values, prompt_index, 0, False).astype(jnp.float32).reshape(PROMPT_LENGTH, KEY_VALUE_HEADS, HEAD_WIDTH)
        place_indices = owner_slot[continuation * MAX_CONT_TILES + jnp.arange(MAX_CONT_TILES, dtype=jnp.int32)]
        self_key_block = continuation_key_slots[place_indices].astype(jnp.float32).reshape(MAX_CONT_TILES * TILE_ROWS, KEY_VALUE_HEADS, HEAD_WIDTH)
        self_value_block = continuation_value_slots[place_indices].astype(jnp.float32).reshape(MAX_CONT_TILES * TILE_ROWS, KEY_VALUE_HEADS, HEAD_WIDTH)
        query_vectors = lax.dynamic_index_in_dim(queries, slot_index, 0, False).astype(jnp.float32).reshape(TILE_ROWS, KEY_VALUE_HEADS, QUERY_HEADS // KEY_VALUE_HEADS, HEAD_WIDTH)
        row_pos = offset + jnp.arange(TILE_ROWS, dtype=jnp.int32)
        col_pos = jnp.arange(MAX_CONT_TILES * TILE_ROWS, dtype=jnp.int32)
        causal = col_pos[None, :] <= row_pos[:, None]
        in_length = row_pos < lengths[continuation]
        per_head = lax.map(partial(group_attention, causal=causal, scaling=scaling), (jnp.moveaxis(query_vectors, 1, 0), jnp.moveaxis(prompt_key_rows, 1, 0), jnp.moveaxis(prompt_value_rows, 1, 0), jnp.moveaxis(self_key_block, 1, 0), jnp.moveaxis(self_value_block, 1, 0)))
        per_head = jnp.transpose(per_head, (2, 0, 1, 3)).reshape(TILE_ROWS, QUERY_HEADS * HEAD_WIDTH)
        return jnp.where(in_length[:, None], per_head, 0.0).astype(jnp.bfloat16)
    attention = lax.map(one_slot, jnp.arange(TILE_SLOTS, dtype=jnp.int32))
    projected = jnp.dot(attention.reshape(TILE_SLOTS * TILE_ROWS, QUERY_HEADS * HEAD_WIDTH), out_weight, preferred_element_type=jnp.float32)
    return projected.astype(jnp.bfloat16).reshape(TILE_SLOTS, TILE_ROWS, D)
```

```python
import functools
import math

import jax
import jax.numpy as jnp
from jax import lax
from jax.experimental import pallas as pl
from jax.experimental.pallas import tpu as pltpu
from jax.sharding import PartitionSpec as P

QUERY_HEADS = 64
KEY_VALUE_HEADS = 8
WIDTH = 128
ROWS = 128
VERY_LOW = -1e30
SCALE = math.log2(math.e) / math.sqrt(WIDTH)
MESH = pl.DeviceIdType.MESH

HEADS_UNIT = 2
UCOLS = HEADS_UNIT * WIDTH
UROWS = HEADS_UNIT * ROWS
CHUNK = 512

PLACES = ((0, 0), (0, 1), (0, 3), (1, 1), (1, 2), (1, 3), (0, 2), (1, 0))
T0, T2, T1, T5, T7, T4, T6, T3 = range(8)
IN67, IN16, IN34, IN35, IN01, IN02, IN03 = range(7)


def across(lhs, rhs):
    return lax.dot_general(lhs, rhs, (((1,), (1,)), ((), ())), preferred_element_type=jnp.float32)


def attend_kernel(
    units,
    lengths, prompts, tiles, q, ck, cv, pk, pv,
    out,
    kall, vall, ckb, cvb, qbuf, obuf, rbuf, lob, lrb, sa, sb, ma, mb, info,
    load_sem, kv_send, kv_recv, q_send, q_recv, o_send, o_recv, l_send, l_recv,
):
    me = lax.axis_index("seq")
    z, y, c = me // 8, (me // 2) % 4, me % 2
    d = 1 - 2 * c
    kd = pk.shape[1]

    def seq(zf, steps):
        return (z + zf) % 2 * 8 + (y + steps * d + 8) % 4 * 2 + c

    def dev(zf, steps):
        return {"seq": seq(zf, steps)}

    other = {"seq": me + d}
    zp, fwd, bwd = dev(1, 0), dev(0, 1), dev(0, -1)

    loads = [
        pltpu.make_async_copy(pk, kall.at[:, pl.ds(0, kd), :], load_sem.at[0]),
        pltpu.make_async_copy(pv, vall.at[:, pl.ds(0, kd), :], load_sem.at[1]),
        pltpu.make_async_copy(ck.at[0], ckb.at[pl.ds(0, ROWS), :], load_sem.at[2]),
        pltpu.make_async_copy(cv.at[0], cvb.at[pl.ds(0, ROWS), :], load_sem.at[3]),
    ] + [
        pltpu.make_async_copy(q.at[0, :, pl.ds(u * UCOLS, UCOLS)], qbuf.at[u], load_sem.at[4 + u])
        for u in range(units)
    ]
    for copy in loads:
        copy.start()

    barrier = pltpu.get_barrier_semaphore()
    for peer in (other, zp, fwd, bwd):
        pl.semaphore_signal(barrier, inc=1, device_id=peer, device_id_type=MESH)
    pl.semaphore_wait(barrier, 4)

    def remote(src, dst, send, recv, to):
        return pltpu.make_async_remote_copy(
            src_ref=src, dst_ref=dst, send_sem=send, recv_sem=recv, device_id=to, device_id_type=MESH
        )

    def kv_copies():
        return [
            remote(ck.at[0], ckb.at[pl.ds(ROWS, ROWS), :], kv_send.at[2], kv_recv.at[2], other),
            remote(pk, kall.at[:, pl.ds(kd, kd), :], kv_send.at[0], kv_recv.at[0], other),
            remote(pv, vall.at[:, pl.ds(kd, kd), :], kv_send.at[1], kv_recv.at[1], other),
            remote(cv.at[0], cvb.at[pl.ds(ROWS, ROWS), :], kv_send.at[3], kv_recv.at[3], other),
        ]

    def q_copy(number, u, place_from, place_to, to):
        src = q.at[0, :, pl.ds(u * UCOLS, UCOLS)] if place_from is None else qbuf.at[place_from * units + u]
        k = place_to * units + u
        return remote(src, qbuf.at[k], q_send.at[number * units + u], q_recv.at[k], to)

    sends0 = []
    for u in range(units):
        sends0 += [
            q_copy(0, u, None, T1, fwd),
            q_copy(1, u, None, T2, bwd),
            q_copy(2, u, None, T3, zp),
        ]
    kvs = kv_copies()
    for copy in sends0[:3]:
        copy.start()
    for copy in kvs:
        copy.start()
    for copy in sends0[3:]:
        copy.start()

    mine, theirs = tiles[me], tiles[me + d]
    for place, (zf, steps) in enumerate(PLACES):
        tile = tiles[seq(zf, steps)]
        info[place, 0] = prompts[tile // 4]
        for k, held in enumerate((mine, theirs)):
            gap = (tile % 2 - held % 2) * ROWS
            info[place, 1 + k] = jnp.where(tile // 2 == held // 2, gap, -4 * ROWS)

    ahead = lax.broadcasted_iota(jnp.int32, (UROWS, ROWS), 1) - (
        lax.broadcasted_iota(jnp.int32, (UROWS, ROWS), 0) % ROWS
    )

    def wait_in(buf, sems, k):
        pltpu.make_async_copy(buf.at[k], buf.at[k], sems.at[k]).wait()

    def o_copy(number, u, place, slot, to):
        k, j = place * units + u, slot * units + u
        return (
            remote(obuf.at[k], rbuf.at[j], o_send.at[number * units + u], o_recv.at[j], to),
            remote(lob.at[k], lrb.at[j], l_send.at[number * units + u], l_recv.at[j], to),
        )

    def send_out(number, u, place, slot, to):
        for copy in o_copy(number, u, place, slot, to):
            copy.start()

    def merged(u, place, slots):
        k = place * units + u
        js = [slot * units + u for slot in slots]
        for j in js:
            wait_in(rbuf, o_recv, j)
            wait_in(lrb, l_recv, j)
        logs = [lob[k]] + [lrb[j] for j in js]
        peak = functools.reduce(jnp.maximum, logs)
        weights = [jnp.exp2(x - peak) for x in logs]
        total = functools.reduce(jnp.add, weights)
        values = [obuf[k]] + [rbuf[j] for j in js]
        parts = []
        for head in range(HEADS_UNIT):
            acc = None
            for w, v in zip(weights, values):
                share = (w / total)[head : head + 1, :]
                column = jnp.broadcast_to(share, (ROWS, ROWS)).T
                term = column * v[:, head * WIDTH : (head + 1) * WIDTH].astype(jnp.float32)
                acc = term if acc is None else acc + term
            parts.append(acc)
        return jnp.concatenate(parts, axis=1), peak + jnp.log2(total)

    def merge_send(number, u, place, slots, slot, to):
        o, log = merged(u, place, slots)
        obuf[place * units + u] = o.astype(jnp.bfloat16)
        lob[place * units + u] = log
        send_out(number, u, place, slot, to)

    def q_ready(n):
        @pl.when(n >= units)
        def _():
            wait_in(qbuf, q_recv, n)

    def relay1(u):
        wait_in(qbuf, q_recv, T1 * units + u)
        q_copy(3, u, T1, T6, fwd).start()
        wait_in(qbuf, q_recv, T3 * units + u)
        q_copy(4, u, T3, T4, fwd).start()
        q_copy(5, u, T3, T5, bwd).start()

    def relay2(u):
        wait_in(qbuf, q_recv, T6 * units + u)
        q_copy(6, u, T6, T7, zp).start()

    waited_by_relay = (T1, T3, T6)

    def before(n):
        @pl.when((n < 2 * units) & (n % 2 == 1))
        def _():
            relay1(n // 2)

        @pl.when((n >= 2 * units) & (n < 4 * units) & (n % 2 == 0))
        def _():
            relay2((n - 2 * units) // 2)

        place = n // units

        @pl.when((place == T2) | (place == T5) | (place == T7) | (place == T4))
        def _():
            wait_in(qbuf, q_recv, n)

    def after(n):
        place, u = n // units, n % units

        @pl.when(place == T2)
        def _():
            send_out(0, u, T2, IN02, fwd)

        @pl.when(place == T5)
        def _():
            send_out(1, u, T5, IN35, fwd)

        @pl.when(place == T7)
        def _():
            send_out(2, u, T7, IN67, zp)

        @pl.when(place == T4)
        def _():
            send_out(3, u, T4, IN34, bwd)

        @pl.when(place == T6)
        def _():
            merge_send(4, u, T6, (IN67,), IN16, bwd)

        @pl.when(place == T3)
        def _():
            merge_send(5, u, T3, (IN34, IN35), IN03, zp)

    chunks = [(i * CHUNK, CHUNK) for i in range(2 * kd // CHUNK)]
    total_keys = 2 * kd

    def fold(op, x):
        parts = [x[:, i : i + 128] for i in range(0, x.shape[1], 128)]
        return functools.reduce(op, parts)

    def both(n1, s1, m1, n2, s2, m2):
        first = n1 is not None
        second = n2 is not None
        if first:
            place1 = n1 // units
            p1 = info[place1, 0]
            raw = qbuf[n1]
            query = jnp.concatenate([raw[:, i * WIDTH : (i + 1) * WIDTH] for i in range(HEADS_UNIT)], axis=0)
            peak = None
        if second:
            p2 = info[n2 // units, 0]
            low = m2[...]
            sums = jnp.zeros((UROWS, 128), jnp.float32)
            acc = jnp.zeros((UROWS, WIDTH), jnp.float32)
        for at, size in chunks + [(total_keys, 2 * ROWS)]:
            own = at >= total_keys
            if first:
                keys = ckb[...] if own else kall[p1, pl.ds(at, size), :]
                s = across(query, keys)
                if own:
                    s = jnp.concatenate(
                        [
                            jnp.where(ahead <= info[place1, 1 + k], s[:, k * ROWS : (k + 1) * ROWS], VERY_LOW)
                            for k in range(2)
                        ],
                        axis=1,
                    )
                s1[:, pl.ds(at, size)] = s
                top = fold(jnp.maximum, s)
                peak = top if peak is None else jnp.maximum(peak, top)
            if second:
                rows = cvb[...] if own else vall[p2, pl.ds(at, size), :]
                w = jnp.exp2(s2[:, pl.ds(at, size)] * SCALE - jnp.concatenate([low] * (size // 128), axis=1))
                sums = sums + fold(jnp.add, w)
                acc = acc + jnp.dot(w.astype(jnp.bfloat16), rows, preferred_element_type=jnp.float32)
        if first:
            m1[...] = jnp.broadcast_to(jnp.max(peak, axis=1, keepdims=True) * SCALE, (UROWS, 128))
        if second:
            total = jnp.sum(sums, axis=1, keepdims=True)
            o = acc / total
            for i in range(HEADS_UNIT):
                obuf[n2, :, i * WIDTH : (i + 1) * WIDTH] = o[i * ROWS : (i + 1) * ROWS].astype(jnp.bfloat16)
            log = low + jnp.log2(total)
            for i in range(HEADS_UNIT):
                lob[n2, i : i + 1, :] = log[i * ROWS : (i + 1) * ROWS].T[0:1, :]

    lob[...] = jnp.zeros_like(lob)
    for copy in loads:
        copy.wait()
    for copy in kvs:
        copy.wait_recv()
    both(0, sa, ma, None, None, None)

    last = 8 * units - 1

    def step(k, carry):
        n = 2 * k
        before(n + 1)
        both(n + 1, sb, mb, n, sa, ma)
        after(n)
        before(jnp.minimum(n + 2, last + 1))
        both(jnp.minimum(n + 2, last), sa, ma, n + 1, sb, mb)
        after(n + 1)
        return carry

    lax.fori_loop(0, 4 * units, step, 0)

    for u in range(units):
        merge_send(6, u, T1, (IN16,), IN01, bwd)

    tile = tiles[me]
    limit = lengths[tile // 4, tile // 2 % 2] - tile % 2 * ROWS
    live = lax.broadcasted_iota(jnp.int32, (ROWS, UCOLS), 0) < limit
    for u in range(units):
        o, _ = merged(u, T0, (IN02, IN03, IN01))
        out[0, :, u * UCOLS : (u + 1) * UCOLS] = jnp.where(live, o, 0.0).astype(jnp.bfloat16)

    for copy in sends0 + kvs:
        copy.wait_send()

    def drain(u, carry):
        for number, src, dst, to in ((3, T1, T6, fwd), (4, T3, T4, fwd), (5, T3, T5, bwd), (6, T6, T7, zp)):
            q_copy(number, u, src, dst, to).wait_send()
        for number, place, slot, to in (
            (0, T2, IN02, fwd), (1, T5, IN35, fwd), (2, T7, IN67, zp), (3, T4, IN34, bwd),
            (4, T6, IN16, bwd), (5, T3, IN03, zp), (6, T1, IN01, bwd),
        ):
            for copy in o_copy(number, u, place, slot, to):
                copy.wait_send()
        return carry

    lax.fori_loop(0, units, drain, 0)


def attend(lengths, prompts, tiles, q, ck, cv, pk, pv):
    units = q.shape[2] // UCOLS
    kd = pk.shape[1]
    keys = 2 * kd + 2 * ROWS
    bf, f32 = jnp.bfloat16, jnp.float32
    smem = pl.BlockSpec(memory_space=pltpu.SMEM)
    hbm = pl.BlockSpec(memory_space=pl.ANY)
    dma = pltpu.SemaphoreType.DMA
    return pl.pallas_call(
        functools.partial(attend_kernel, units),
        out_shape=jax.ShapeDtypeStruct(q.shape, bf),
        in_specs=[smem] * 3 + [hbm] * 5,
        out_specs=pl.BlockSpec(memory_space=pltpu.VMEM),
        scratch_shapes=[
            pltpu.VMEM((2, 2 * kd, WIDTH), bf),
            pltpu.VMEM((2, 2 * kd, WIDTH), bf),
            pltpu.VMEM((2 * ROWS, WIDTH), bf),
            pltpu.VMEM((2 * ROWS, WIDTH), bf),
            pltpu.VMEM((8 * units, ROWS, UCOLS), bf),
            pltpu.VMEM((8 * units, ROWS, UCOLS), bf),
            pltpu.VMEM((7 * units, ROWS, UCOLS), bf),
            pltpu.VMEM((8 * units, 8, ROWS), f32),
            pltpu.VMEM((7 * units, 8, ROWS), f32),
            pltpu.VMEM((UROWS, keys), f32),
            pltpu.VMEM((UROWS, keys), f32),
            pltpu.VMEM((UROWS, 128), f32),
            pltpu.VMEM((UROWS, 128), f32),
            pltpu.SMEM((8, 4), jnp.int32),
            dma((4 + units,)),
            dma((4,)),
            dma((4,)),
            dma((7 * units,)),
            dma((8 * units,)),
            dma((7 * units,)),
            dma((7 * units,)),
            dma((7 * units,)),
            dma((7 * units,)),
        ],
        compiler_params=pltpu.CompilerParams(
            collective_id=0, has_side_effects=True, vmem_limit_bytes=48 << 20
        ),
        name="attend",
    )(lengths, prompts, tiles, q, ck, cv, pk, pv)


def split_up(x, dim, length):
    before, after = (x.shape[:dim], x.shape[dim + 1 :])
    return jnp.moveaxis(x.reshape(*before, length, -1, *after), dim, 0)


def summed_on_arrival(x, axis, dim):
    length = lax.axis_size(axis)
    blocks = lax.all_to_all(split_up(x, dim, length), axis, 0, 0, tiled=True)
    return jnp.sum(blocks.astype(jnp.float32), axis=0)


def local(q, ck, cv, pk, pv, lengths, prompts, tiles, weight):
    attention = attend(lengths, prompts, tiles, q, ck, cv, pk, pv)
    partial_out = jnp.einsum(
        "stc,cd->std",
        lax.all_gather(attention, "seq", axis=0, tiled=True),
        weight,
        preferred_element_type=jnp.float32,
    )
    return summed_on_arrival(partial_out.astype(jnp.bfloat16), "head", 0).astype(jnp.bfloat16)


def solution(mesh):
    return jax.shard_map(
        local,
        mesh=mesh,
        in_specs=(
            P("seq", None, "head"),
            P("seq", None, "head"),
            P("seq", None, "head"),
            P(None, "seq", "head"),
            P(None, "seq", "head"),
            P(),
            P(),
            P(),
            P("head", "seq"),
        ),
        out_specs=P("head", None, "seq"),
        check_vma=False,
    )
```

```python
import functools
import math

import jax
import jax.numpy as jnp
from jax import lax
from jax.experimental import pallas as pl
from jax.experimental.pallas import tpu as pltpu
from jax.sharding import PartitionSpec as P

QUERY_HEADS = 64
KEY_VALUE_HEADS = 8
WIDTH = 128
ROWS = 128
VERY_LOW = -1e30
SCALE = math.log2(math.e) / math.sqrt(WIDTH)
MESH = pl.DeviceIdType.MESH

HEADS_UNIT = 2
UCOLS = HEADS_UNIT * WIDTH
UROWS = HEADS_UNIT * ROWS
CHUNK = 512

PLACES = ((0, 0), (0, 1), (0, 3), (1, 1), (1, 2), (1, 3), (0, 2), (1, 0))
T0, T2, T1, T5, T7, T4, T6, T3 = range(8)
IN67, IN16, IN34, IN35, IN01, IN02, IN03 = range(7)


def across(lhs, rhs):
    return lax.dot_general(lhs, rhs, (((1,), (1,)), ((), ())), preferred_element_type=jnp.float32)


def attend_kernel(
    units,
    lengths, prompts, tiles, q, ck, cv, pk, pv, weight,
    out,
    kall, vall, ckb, cvb, qbuf, obuf, rbuf, lob, lrb, sa, sb, ma, mb, info,
    wbuf, abuf, pbuf, far_in, leaf_in, inter_in, zin, zout, fin, xout,
    load_sem, kv_send, kv_recv, q_send, q_recv, o_send, o_recv, l_send, l_recv,
    a_send, a_recv, far_send, far_recv, leaf_send, leaf_recv, inter_send, inter_recv, z_send, z_recv, x_sem,
):
    me = lax.axis_index("seq")
    z, y, c = me // 8, (me // 2) % 4, me % 2
    d = 1 - 2 * c
    kd = pk.shape[1]

    def seq(zf, steps):
        return (z + zf) % 2 * 8 + (y + steps * d + 8) % 4 * 2 + c

    def dev(zf, steps):
        return {"seq": seq(zf, steps)}

    other = {"seq": me + d}
    zp, fwd, bwd = dev(1, 0), dev(0, 1), dev(0, -1)
    group = lax.axis_index("head")
    x, zh = group // 2, group % 2
    xfwd = {"head": (x + d + 4) % 4 * 2 + zh}
    xbwd = {"head": (x - d + 4) % 4 * 2 + zh}
    zhp = {"head": x * 2 + 1 - zh}

    loads = [
        pltpu.make_async_copy(pk, kall.at[:, pl.ds(0, kd), :], load_sem.at[0]),
        pltpu.make_async_copy(pv, vall.at[:, pl.ds(0, kd), :], load_sem.at[1]),
        pltpu.make_async_copy(ck.at[0], ckb.at[pl.ds(0, ROWS), :], load_sem.at[2]),
        pltpu.make_async_copy(cv.at[0], cvb.at[pl.ds(0, ROWS), :], load_sem.at[3]),
    ] + [
        pltpu.make_async_copy(q.at[0, :, pl.ds(u * UCOLS, UCOLS)], qbuf.at[u], load_sem.at[4 + u])
        for u in range(units)
    ]
    wload = pltpu.make_async_copy(weight, wbuf.at[c], load_sem.at[4 + units])
    for copy in loads:
        copy.start()

    barrier = pltpu.get_barrier_semaphore()
    for peer in (other, zp, fwd, bwd, xfwd, xbwd, zhp):
        pl.semaphore_signal(barrier, inc=1, device_id=peer, device_id_type=MESH)
    pl.semaphore_wait(barrier, 7)

    def remote(src, dst, send, recv, to):
        return pltpu.make_async_remote_copy(
            src_ref=src, dst_ref=dst, send_sem=send, recv_sem=recv, device_id=to, device_id_type=MESH
        )

    def kv_copies():
        return [
            remote(ck.at[0], ckb.at[pl.ds(ROWS, ROWS), :], kv_send.at[2], kv_recv.at[2], other),
            remote(pk, kall.at[:, pl.ds(kd, kd), :], kv_send.at[0], kv_recv.at[0], other),
            remote(pv, vall.at[:, pl.ds(kd, kd), :], kv_send.at[1], kv_recv.at[1], other),
            remote(cv.at[0], cvb.at[pl.ds(ROWS, ROWS), :], kv_send.at[3], kv_recv.at[3], other),
        ]

    wsend = remote(weight, wbuf.at[c], kv_send.at[4], kv_recv.at[4], other)

    def q_copy(number, u, place_from, place_to, to):
        src = q.at[0, :, pl.ds(u * UCOLS, UCOLS)] if place_from is None else qbuf.at[place_from * units + u]
        k = place_to * units + u
        return remote(src, qbuf.at[k], q_send.at[number * units + u], q_recv.at[k], to)

    sends0 = []
    for u in range(units):
        sends0 += [
            q_copy(0, u, None, T1, fwd),
            q_copy(1, u, None, T2, bwd),
            q_copy(2, u, None, T3, zp),
        ]
    kvs = kv_copies()
    for copy in sends0[:3]:
        copy.start()
    for copy in kvs:
        copy.start()
    for copy in sends0[3:]:
        copy.start()
    wload.start()
    wsend.start()

    mine, theirs = tiles[me], tiles[me + d]
    for place, (zf, steps) in enumerate(PLACES):
        tile = tiles[seq(zf, steps)]
        info[place, 0] = prompts[tile // 4]
        for k, held in enumerate((mine, theirs)):
            gap = (tile % 2 - held % 2) * ROWS
            info[place, 1 + k] = jnp.where(tile // 2 == held // 2, gap, -4 * ROWS)

    ahead = lax.broadcasted_iota(jnp.int32, (UROWS, ROWS), 1) - (
        lax.broadcasted_iota(jnp.int32, (UROWS, ROWS), 0) % ROWS
    )

    def wait_in(buf, sems, k):
        pltpu.make_async_copy(buf.at[k], buf.at[k], sems.at[k]).wait()

    def o_copy(number, u, place, slot, to):
        k, j = place * units + u, slot * units + u
        return (
            remote(obuf.at[k], rbuf.at[j], o_send.at[number * units + u], o_recv.at[j], to),
            remote(lob.at[k], lrb.at[j], l_send.at[number * units + u], l_recv.at[j], to),
        )

    def send_out(number, u, place, slot, to):
        for copy in o_copy(number, u, place, slot, to):
            copy.start()

    def merged(u, place, slots):
        k = place * units + u
        js = [slot * units + u for slot in slots]
        for j in js:
            wait_in(rbuf, o_recv, j)
            wait_in(lrb, l_recv, j)
        logs = [lob[k]] + [lrb[j] for j in js]
        peak = functools.reduce(jnp.maximum, logs)
        weights = [jnp.exp2(x - peak) for x in logs]
        total = functools.reduce(jnp.add, weights)
        values = [obuf[k]] + [rbuf[j] for j in js]
        parts = []
        for head in range(HEADS_UNIT):
            acc = None
            for w, v in zip(weights, values):
                share = (w / total)[head : head + 1, :]
                column = jnp.broadcast_to(share, (ROWS, ROWS)).T
                term = column * v[:, head * WIDTH : (head + 1) * WIDTH].astype(jnp.float32)
                acc = term if acc is None else acc + term
            parts.append(acc)
        return jnp.concatenate(parts, axis=1), peak + jnp.log2(total)

    def merge_send(number, u, place, slots, slot, to):
        o, log = merged(u, place, slots)
        obuf[place * units + u] = o.astype(jnp.bfloat16)
        lob[place * units + u] = log
        send_out(number, u, place, slot, to)

    def q_ready(n):
        @pl.when(n >= units)
        def _():
            wait_in(qbuf, q_recv, n)

    def relay1(u):
        wait_in(qbuf, q_recv, T1 * units + u)
        q_copy(3, u, T1, T6, fwd).start()
        wait_in(qbuf, q_recv, T3 * units + u)
        q_copy(4, u, T3, T4, fwd).start()
        q_copy(5, u, T3, T5, bwd).start()

    def relay2(u):
        wait_in(qbuf, q_recv, T6 * units + u)
        q_copy(6, u, T6, T7, zp).start()

    waited_by_relay = (T1, T3, T6)

    def before(n):
        @pl.when((n < 2 * units) & (n % 2 == 1))
        def _():
            relay1(n // 2)

        @pl.when((n >= 2 * units) & (n < 4 * units) & (n % 2 == 0))
        def _():
            relay2((n - 2 * units) // 2)

        place = n // units

        @pl.when((place == T2) | (place == T5) | (place == T7) | (place == T4))
        def _():
            wait_in(qbuf, q_recv, n)

    def after(n):
        place, u = n // units, n % units

        @pl.when(place == T2)
        def _():
            send_out(0, u, T2, IN02, fwd)

        @pl.when(place == T5)
        def _():
            send_out(1, u, T5, IN35, fwd)

        @pl.when(place == T7)
        def _():
            send_out(2, u, T7, IN67, zp)

        @pl.when(place == T4)
        def _():
            send_out(3, u, T4, IN34, bwd)

        @pl.when(place == T6)
        def _():
            merge_send(4, u, T6, (IN67,), IN16, bwd)

        @pl.when(place == T3)
        def _():
            merge_send(5, u, T3, (IN34, IN35), IN03, zp)

    chunks = [(i * CHUNK, CHUNK) for i in range(2 * kd // CHUNK)]
    total_keys = 2 * kd

    def fold(op, x):
        parts = [x[:, i : i + 128] for i in range(0, x.shape[1], 128)]
        return functools.reduce(op, parts)

    def both(n1, s1, m1, n2, s2, m2):
        first = n1 is not None
        second = n2 is not None
        if first:
            place1 = n1 // units
            p1 = info[place1, 0]
            raw = qbuf[n1]
            query = jnp.concatenate([raw[:, i * WIDTH : (i + 1) * WIDTH] for i in range(HEADS_UNIT)], axis=0)
            peak = None
        if second:
            p2 = info[n2 // units, 0]
            low = m2[...]
            sums = jnp.zeros((UROWS, 128), jnp.float32)
            acc = jnp.zeros((UROWS, WIDTH), jnp.float32)
        for at, size in chunks + [(total_keys, 2 * ROWS)]:
            own = at >= total_keys
            if first:
                keys = ckb[...] if own else kall[p1, pl.ds(at, size), :]
                s = across(query, keys)
                if own:
                    s = jnp.concatenate(
                        [
                            jnp.where(ahead <= info[place1, 1 + k], s[:, k * ROWS : (k + 1) * ROWS], VERY_LOW)
                            for k in range(2)
                        ],
                        axis=1,
                    )
                s1[:, pl.ds(at, size)] = s
                top = fold(jnp.maximum, s)
                peak = top if peak is None else jnp.maximum(peak, top)
            if second:
                rows = cvb[...] if own else vall[p2, pl.ds(at, size), :]
                w = jnp.exp2(s2[:, pl.ds(at, size)] * SCALE - jnp.concatenate([low] * (size // 128), axis=1))
                sums = sums + fold(jnp.add, w)
                acc = acc + jnp.dot(w.astype(jnp.bfloat16), rows, preferred_element_type=jnp.float32)
        if first:
            m1[...] = jnp.broadcast_to(jnp.max(peak, axis=1, keepdims=True) * SCALE, (UROWS, 128))
        if second:
            total = jnp.sum(sums, axis=1, keepdims=True)
            o = acc / total
            for i in range(HEADS_UNIT):
                obuf[n2, :, i * WIDTH : (i + 1) * WIDTH] = o[i * ROWS : (i + 1) * ROWS].astype(jnp.bfloat16)
            log = low + jnp.log2(total)
            for i in range(HEADS_UNIT):
                lob[n2, i : i + 1, :] = log[i * ROWS : (i + 1) * ROWS].T[0:1, :]

    lob[...] = jnp.zeros_like(lob)
    for copy in loads:
        copy.wait()
    for copy in kvs:
        copy.wait_recv()
    both(0, sa, ma, None, None, None)

    last = 8 * units - 1

    def step(k, carry):
        n = 2 * k
        before(n + 1)
        both(n + 1, sb, mb, n, sa, ma)
        after(n)
        before(jnp.minimum(n + 2, last + 1))
        both(jnp.minimum(n + 2, last), sa, ma, n + 1, sb, mb)
        after(n + 1)
        return carry

    lax.fori_loop(0, 4 * units, step, 0)

    for u in range(units):
        merge_send(6, u, T1, (IN16,), IN01, bwd)

    def a_copy(number, u, place_from, place_to, to):
        k = place_to * units + u
        return remote(
            abuf.at[place_from * units + u], abuf.at[k], a_send.at[number * units + u], a_recv.at[k], to
        )

    def a_relay1(u):
        wait_in(abuf, a_recv, T1 * units + u)
        a_copy(3, u, T1, T6, fwd).start()
        wait_in(abuf, a_recv, T3 * units + u)
        a_copy(4, u, T3, T4, fwd).start()
        a_copy(5, u, T3, T5, bwd).start()

    def a_relay2(u):
        wait_in(abuf, a_recv, T6 * units + u)
        a_copy(6, u, T6, T7, zp).start()

    tile = tiles[me]
    limit = lengths[tile // 4, tile // 2 % 2] - tile % 2 * ROWS
    live = lax.broadcasted_iota(jnp.int32, (ROWS, UCOLS), 0) < limit
    for u in range(units):
        o, _ = merged(u, T0, (IN02, IN03, IN01))
        abuf[T0 * units + u] = jnp.where(live, o, 0.0).astype(jnp.bfloat16)
        a_copy(0, u, T0, T1, fwd).start()
        a_copy(1, u, T0, T2, bwd).start()
        a_copy(2, u, T0, T3, zp).start()

    def far_copy(zt, part, source):
        k = zt * 2 + part
        return remote(pbuf.at[source * 2 + part], far_in.at[k], far_send.at[k], far_recv.at[k], xbwd)

    def leaf_copy(zt, part, source):
        k = zt * 2 + part
        return remote(pbuf.at[source * 2 + part], leaf_in.at[k], leaf_send.at[k], leaf_recv.at[k], xfwd)

    def inter_copy(zt, part, source):
        k = zt * 2 + part
        return remote(pbuf.at[source * 2 + part], inter_in.at[k], inter_send.at[k], inter_recv.at[k], xbwd)

    def project(place):
        zf, steps = PLACES[place]
        home = seq(zf, steps) // 2
        rows = jnp.concatenate([abuf[place * units + u] for u in range(units)], axis=1)
        for part in range(2):
            pbuf[home * 2 + part] = jnp.dot(rows, wbuf[part], preferred_element_type=jnp.float32).astype(
                jnp.bfloat16
            )
        gap = (home // 2 - x + 4) % 4

        @pl.when(gap == 2)
        def _():
            for part in range(2):
                far_copy(home % 2, part, home).start()

        @pl.when(gap == (d + 4) % 4)
        def _():
            for part in range(2):
                leaf_copy(home % 2, part, home).start()

    def settle(place):
        for u in range(units):
            wait_in(abuf, a_recv, place * units + u)

    wload.wait()
    wsend.wait_recv()
    project(T0)
    for u in range(units):
        a_relay1(u)
    project(T1)
    project(T3)
    settle(T2)
    project(T2)
    for u in range(units):
        a_relay2(u)
    project(T6)
    settle(T5)
    project(T5)
    settle(T4)
    project(T4)
    settle(T7)
    project(T7)

    f32 = jnp.float32
    inter_home = (x - d + 4) % 4 * 2
    for zt in (1 - zh, zh):
        for part in range(2):
            k, m = zt * 2 + part, (inter_home + zt) * 2 + part
            wait_in(far_in, far_recv, k)
            pbuf[m] = (pbuf[m].astype(f32) + far_in[k].astype(f32)).astype(jnp.bfloat16)
            inter_copy(zt, part, inter_home + zt).start()

    def column_sum(zt, part):
        k = zt * 2 + part
        wait_in(leaf_in, leaf_recv, k)
        wait_in(inter_in, inter_recv, k)
        here = pbuf[(x * 2 + zt) * 2 + part].astype(f32)
        return here + leaf_in[k].astype(f32) + inter_in[k].astype(f32)

    def z_copy(part):
        return remote(zout.at[part], zin.at[part], z_send.at[part], z_recv.at[part], zhp)

    for part in range(2):
        zout[part] = column_sum(1 - zh, part).astype(jnp.bfloat16)
        z_copy(part).start()
    for part in range(2):
        fin[part] = column_sum(zh, part)
    for part in range(2):
        wait_in(zin, z_recv, part)
    xout[...] = (fin[1 - c] + zin[1 - c].astype(f32)).astype(jnp.bfloat16)
    last_copy = remote(xout, out.at[c], x_sem.at[0], x_sem.at[1], other)
    last_copy.start()
    out[c] = (fin[c] + zin[c].astype(f32)).astype(jnp.bfloat16)
    last_copy.wait()

    for copy in sends0 + kvs + [wsend]:
        copy.wait_send()
    for part in range(2):
        z_copy(part).wait_send()
        for zt in range(2):
            far_copy(zt, part, 0).wait_send()
            leaf_copy(zt, part, 0).wait_send()
            inter_copy(zt, part, 0).wait_send()

    def drain(u, carry):
        for make in (q_copy, a_copy):
            for number, src, dst, to in ((3, T1, T6, fwd), (4, T3, T4, fwd), (5, T3, T5, bwd), (6, T6, T7, zp)):
                make(number, u, src, dst, to).wait_send()
        for number, dst, to in ((0, T1, fwd), (1, T2, bwd), (2, T3, zp)):
            a_copy(number, u, T0, dst, to).wait_send()
        for number, place, slot, to in (
            (0, T2, IN02, fwd), (1, T5, IN35, fwd), (2, T7, IN67, zp), (3, T4, IN34, bwd),
            (4, T6, IN16, bwd), (5, T3, IN03, zp), (6, T1, IN01, bwd),
        ):
            for copy in o_copy(number, u, place, slot, to):
                copy.wait_send()
        return carry

    lax.fori_loop(0, units, drain, 0)


def attend(lengths, prompts, tiles, q, ck, cv, pk, pv, weight):
    units = q.shape[2] // UCOLS
    kd = pk.shape[1]
    cols = weight.shape[1]
    keys = 2 * kd + 2 * ROWS
    bf, f32 = jnp.bfloat16, jnp.float32
    smem = pl.BlockSpec(memory_space=pltpu.SMEM)
    hbm = pl.BlockSpec(memory_space=pl.ANY)
    dma = pltpu.SemaphoreType.DMA
    return pl.pallas_call(
        functools.partial(attend_kernel, units),
        out_shape=jax.ShapeDtypeStruct((2, ROWS, weight.shape[1]), bf),
        in_specs=[smem] * 3 + [hbm] * 6,
        out_specs=pl.BlockSpec(memory_space=pltpu.VMEM),
        scratch_shapes=[
            pltpu.VMEM((2, 2 * kd, WIDTH), bf),
            pltpu.VMEM((2, 2 * kd, WIDTH), bf),
            pltpu.VMEM((2 * ROWS, WIDTH), bf),
            pltpu.VMEM((2 * ROWS, WIDTH), bf),
            pltpu.VMEM((8 * units, ROWS, UCOLS), bf),
            pltpu.VMEM((8 * units, ROWS, UCOLS), bf),
            pltpu.VMEM((7 * units, ROWS, UCOLS), bf),
            pltpu.VMEM((8 * units, 8, ROWS), f32),
            pltpu.VMEM((7 * units, 8, ROWS), f32),
            pltpu.VMEM((UROWS, keys), f32),
            pltpu.VMEM((UROWS, keys), f32),
            pltpu.VMEM((UROWS, 128), f32),
            pltpu.VMEM((UROWS, 128), f32),
            pltpu.SMEM((8, 4), jnp.int32),
            pltpu.VMEM((2,) + weight.shape, bf),
            pltpu.VMEM((8 * units, ROWS, UCOLS), bf),
            pltpu.VMEM((16, ROWS, cols), bf),
            pltpu.VMEM((4, ROWS, cols), bf),
            pltpu.VMEM((4, ROWS, cols), bf),
            pltpu.VMEM((4, ROWS, cols), bf),
            pltpu.VMEM((2, ROWS, cols), bf),
            pltpu.VMEM((2, ROWS, cols), bf),
            pltpu.VMEM((2, ROWS, cols), f32),
            pltpu.VMEM((ROWS, cols), bf),
            dma((5 + units,)),
            dma((5,)),
            dma((5,)),
            dma((7 * units,)),
            dma((8 * units,)),
            dma((7 * units,)),
            dma((7 * units,)),
            dma((7 * units,)),
            dma((7 * units,)),
            dma((7 * units,)),
            dma((8 * units,)),
            dma((4,)),
            dma((4,)),
            dma((4,)),
            dma((4,)),
            dma((4,)),
            dma((4,)),
            dma((2,)),
            dma((2,)),
            dma((2,)),
        ],
        compiler_params=pltpu.CompilerParams(
            collective_id=0, has_side_effects=True, vmem_limit_bytes=60 << 20
        ),
        name="attend",
    )(lengths, prompts, tiles, q, ck, cv, pk, pv, weight)


def local(q, ck, cv, pk, pv, lengths, prompts, tiles, weight):
    return attend(lengths, prompts, tiles, q, ck, cv, pk, pv, weight)


def solution(mesh):
    return jax.shard_map(
        local,
        mesh=mesh,
        in_specs=(
            P("seq", None, "head"),
            P("seq", None, "head"),
            P("seq", None, "head"),
            P(None, "seq", "head"),
            P(None, "seq", "head"),
            P(),
            P(),
            P(),
            P("head", "seq"),
        ),
        out_specs=P("head", None, "seq"),
        check_vma=False,
    )
```

```python
import functools
import math

import jax
import jax.numpy as jnp
from jax import lax
from jax.experimental import pallas as pl
from jax.experimental.pallas import tpu as pltpu
from jax.sharding import PartitionSpec as P

QUERY_HEADS = 64
KEY_VALUE_HEADS = 8
WIDTH = 128
ROWS = 128
VERY_LOW = -1e30
SCALE = math.log2(math.e) / math.sqrt(WIDTH)
MESH = pl.DeviceIdType.MESH

HEADS_UNIT = 2
UCOLS = HEADS_UNIT * WIDTH
UROWS = HEADS_UNIT * ROWS
CHUNK = 512

PLACES = ((0, 0), (0, 1), (0, 3), (1, 1), (1, 2), (1, 3), (0, 2), (1, 0))
T0, T2, T1, T5, T7, T4, T6, T3 = range(8)
IN67, IN16, IN34, IN35, IN01, IN02, IN03 = range(7)


def across(lhs, rhs):
    return lax.dot_general(lhs, rhs, (((1,), (1,)), ((), ())), preferred_element_type=jnp.float32)


def attend_kernel(
    units,
    lengths, prompts, tiles, q, ck, cv, pk, pv, weight,
    out,
    kall, vall, ckb, cvb, qbuf, obuf, rbuf, lob, lrb, sa, sb, ma, mb, low_a, low_b, sums_a, sums_b, acc_a, acc_b, info,
    wbuf, abuf, pbuf, far_in, leaf_in, inter_in, zin, zout, fin, xout,
    load_sem, kv_send, kv_recv, q_send, q_recv, o_send, o_recv, l_send, l_recv,
    a_send, a_recv, far_send, far_recv, leaf_send, leaf_recv, inter_send, inter_recv, z_send, z_recv, x_sem,
):
    me = lax.axis_index("seq")
    z, y, c = me // 8, (me // 2) % 4, me % 2
    d = 1 - 2 * c
    kd = pk.shape[1]

    def seq(zf, steps):
        return (z + zf) % 2 * 8 + (y + steps * d + 8) % 4 * 2 + c

    def dev(zf, steps):
        return {"seq": seq(zf, steps)}

    other = {"seq": me + d}
    zp, fwd, bwd = dev(1, 0), dev(0, 1), dev(0, -1)
    group = lax.axis_index("head")
    x, zh = group // 2, group % 2
    xfwd = {"head": (x + d + 4) % 4 * 2 + zh}
    xbwd = {"head": (x - d + 4) % 4 * 2 + zh}
    zhp = {"head": x * 2 + 1 - zh}

    loads = [
        pltpu.make_async_copy(pk, kall.at[:, pl.ds(0, kd), :], load_sem.at[0]),
        pltpu.make_async_copy(pv, vall.at[:, pl.ds(0, kd), :], load_sem.at[1]),
        pltpu.make_async_copy(ck.at[0], ckb.at[pl.ds(0, ROWS), :], load_sem.at[2]),
        pltpu.make_async_copy(cv.at[0], cvb.at[pl.ds(0, ROWS), :], load_sem.at[3]),
    ] + [
        pltpu.make_async_copy(q.at[0, :, pl.ds(u * UCOLS, UCOLS)], qbuf.at[u], load_sem.at[4 + u])
        for u in range(units)
    ]
    wload = pltpu.make_async_copy(weight, wbuf.at[c], load_sem.at[4 + units])
    for copy in loads:
        copy.start()

    barrier = pltpu.get_barrier_semaphore()
    for peer in (other, zp, fwd, bwd, xfwd, xbwd, zhp):
        pl.semaphore_signal(barrier, inc=1, device_id=peer, device_id_type=MESH)
    pl.semaphore_wait(barrier, 7)

    def remote(src, dst, send, recv, to):
        return pltpu.make_async_remote_copy(
            src_ref=src, dst_ref=dst, send_sem=send, recv_sem=recv, device_id=to, device_id_type=MESH
        )

    def kv_copies():
        return [
            remote(ck.at[0], ckb.at[pl.ds(ROWS, ROWS), :], kv_send.at[2], kv_recv.at[2], other),
            remote(pk, kall.at[:, pl.ds(kd, kd), :], kv_send.at[0], kv_recv.at[0], other),
            remote(pv, vall.at[:, pl.ds(kd, kd), :], kv_send.at[1], kv_recv.at[1], other),
            remote(cv.at[0], cvb.at[pl.ds(ROWS, ROWS), :], kv_send.at[3], kv_recv.at[3], other),
        ]

    wsend = remote(weight, wbuf.at[c], kv_send.at[4], kv_recv.at[4], other)

    def q_copy(number, u, place_from, place_to, to):
        src = q.at[0, :, pl.ds(u * UCOLS, UCOLS)] if place_from is None else qbuf.at[place_from * units + u]
        k = place_to * units + u
        return remote(src, qbuf.at[k], q_send.at[number * units + u], q_recv.at[k], to)

    sends0 = []
    for u in range(units):
        sends0 += [
            q_copy(0, u, None, T1, fwd),
            q_copy(1, u, None, T2, bwd),
            q_copy(2, u, None, T3, zp),
        ]
    kvs = kv_copies()
    for copy in sends0[:3]:
        copy.start()
    for copy in kvs:
        copy.start()
    for copy in sends0[3:]:
        copy.start()
    wload.start()
    wsend.start()

    mine, theirs = tiles[me], tiles[me + d]
    for place, (zf, steps) in enumerate(PLACES):
        tile = tiles[seq(zf, steps)]
        info[place, 0] = prompts[tile // 4]
        for k, held in enumerate((mine, theirs)):
            gap = (tile % 2 - held % 2) * ROWS
            info[place, 1 + k] = jnp.where(tile // 2 == held // 2, gap, -4 * ROWS)

    ahead = lax.broadcasted_iota(jnp.int32, (UROWS, ROWS), 1) - (
        lax.broadcasted_iota(jnp.int32, (UROWS, ROWS), 0) % ROWS
    )

    def wait_in(buf, sems, k):
        pltpu.make_async_copy(buf.at[k], buf.at[k], sems.at[k]).wait()

    def o_copy(number, u, place, slot, to):
        k, j = place * units + u, slot * units + u
        return (
            remote(obuf.at[k], rbuf.at[j], o_send.at[number * units + u], o_recv.at[j], to),
            remote(lob.at[k], lrb.at[j], l_send.at[number * units + u], l_recv.at[j], to),
        )

    def send_out(number, u, place, slot, to):
        for copy in o_copy(number, u, place, slot, to):
            copy.start()

    def merged(u, place, slots):
        k = place * units + u
        js = [slot * units + u for slot in slots]
        for j in js:
            wait_in(rbuf, o_recv, j)
            wait_in(lrb, l_recv, j)
        logs = [lob[k]] + [lrb[j] for j in js]
        peak = functools.reduce(jnp.maximum, logs)
        weights = [jnp.exp2(x - peak) for x in logs]
        total = functools.reduce(jnp.add, weights)
        values = [obuf[k]] + [rbuf[j] for j in js]
        parts = []
        for head in range(HEADS_UNIT):
            acc = None
            for w, v in zip(weights, values):
                share = (w / total)[head : head + 1, :]
                column = jnp.broadcast_to(share, (ROWS, ROWS)).T
                term = column * v[:, head * WIDTH : (head + 1) * WIDTH].astype(jnp.float32)
                acc = term if acc is None else acc + term
            parts.append(acc)
        return jnp.concatenate(parts, axis=1), peak + jnp.log2(total)

    def merge_send(number, u, place, slots, slot, to):
        o, log = merged(u, place, slots)
        obuf[place * units + u] = o.astype(jnp.bfloat16)
        lob[place * units + u] = log
        send_out(number, u, place, slot, to)

    def relay1(u):
        wait_in(qbuf, q_recv, T1 * units + u)
        q_copy(3, u, T1, T6, fwd).start()
        wait_in(qbuf, q_recv, T3 * units + u)
        q_copy(4, u, T3, T4, fwd).start()
        q_copy(5, u, T3, T5, bwd).start()

    def relay2(u):
        wait_in(qbuf, q_recv, T6 * units + u)
        q_copy(6, u, T6, T7, zp).start()

    def before(k):
        @pl.when(k < units)
        def _():
            relay1(k)

        @pl.when((k >= units) & (k < 2 * units))
        def _():
            relay2(k - units)

        for ahead_by in (1, 2):
            n = 2 * k + ahead_by
            place = n // units

            @pl.when((place == T2) | (place == T5) | (place == T7) | (place == T4))
            def _():
                wait_in(qbuf, q_recv, n)

    def after(n):
        place, u = n // units, n % units

        @pl.when(place == T2)
        def _():
            send_out(0, u, T2, IN02, fwd)

        @pl.when(place == T5)
        def _():
            send_out(1, u, T5, IN35, fwd)

        @pl.when(place == T7)
        def _():
            send_out(2, u, T7, IN67, zp)

        @pl.when(place == T4)
        def _():
            send_out(3, u, T4, IN34, bwd)

        @pl.when(place == T6)
        def _():
            merge_send(4, u, T6, (IN67,), IN16, bwd)

        @pl.when(place == T3)
        def _():
            merge_send(5, u, T3, (IN34, IN35), IN03, zp)

    chunks = [(i * CHUNK, CHUNK) for i in range(2 * kd // CHUNK)]
    total_keys = 2 * kd

    def fold(op, x):
        parts = [x[:, i : i + 128] for i in range(0, x.shape[1], 128)]
        return functools.reduce(op, parts)

    def both(n1, s1, m1, n2, s2, m2, low2, sums2, acc2):
        first = n1 is not None
        second = n2 is not None
        if first:
            place1 = n1 // units
            p1 = info[place1, 0]
            raw = qbuf[n1]
            query = jnp.concatenate([raw[:, i * WIDTH : (i + 1) * WIDTH] for i in range(HEADS_UNIT)], axis=0)
            peak = None
        if second:
            p2 = info[n2 // units, 0]
            low = jnp.broadcast_to(jnp.max(m2[...], axis=1, keepdims=True) * SCALE, (UROWS, 128))
            sums = jnp.zeros((UROWS, 128), jnp.float32)
            acc = jnp.zeros((UROWS, WIDTH), jnp.float32)
        for at, size in chunks + [(total_keys, 2 * ROWS)]:
            own = at >= total_keys
            if first:
                keys = ckb[...] if own else kall[p1, pl.ds(at, size), :]
                s = across(query, keys)
                if own:
                    s = jnp.concatenate(
                        [
                            jnp.where(ahead <= info[place1, 1 + k], s[:, k * ROWS : (k + 1) * ROWS], VERY_LOW)
                            for k in range(2)
                        ],
                        axis=1,
                    )
                s1[:, pl.ds(at, size)] = s
                top = fold(jnp.maximum, s)
                peak = top if peak is None else jnp.maximum(peak, top)
            if second:
                rows = cvb[...] if own else vall[p2, pl.ds(at, size), :]
                w = jnp.exp2(s2[:, pl.ds(at, size)] * SCALE - jnp.concatenate([low] * (size // 128), axis=1))
                sums = sums + fold(jnp.add, w)
                acc = acc + jnp.dot(w.astype(jnp.bfloat16), rows, preferred_element_type=jnp.float32)
        if first:
            m1[...] = peak
        if second:
            low2[...] = low
            sums2[...] = sums
            acc2[...] = acc

    def finish(n, low2, sums2, acc2):
        total = jnp.sum(sums2[...], axis=1, keepdims=True)
        o = acc2[...] / total
        log = low2[...] + jnp.log2(total)
        for i in range(HEADS_UNIT):
            obuf[n, :, i * WIDTH : (i + 1) * WIDTH] = o[i * ROWS : (i + 1) * ROWS].astype(jnp.bfloat16)
            lob[n, i : i + 1, :] = log[i * ROWS : (i + 1) * ROWS].T[0:1, :]

    lob[...] = jnp.zeros_like(lob)
    sums_b[...] = jnp.ones_like(sums_b)
    for copy in loads:
        copy.wait()
    for copy in kvs:
        copy.wait_recv()
    both(0, sa, ma, None, None, None, None, None, None)

    last = 8 * units - 1

    def step(k, carry):
        n = 2 * k
        before(k)
        finish(jnp.maximum(n - 1, 0), low_b, sums_b, acc_b)
        both(n + 1, sb, mb, n, sa, ma, low_a, sums_a, acc_a)
        finish(n, low_a, sums_a, acc_a)
        both(jnp.minimum(n + 2, last), sa, ma, n + 1, sb, mb, low_b, sums_b, acc_b)
        after(n - 1)
        after(n)
        return carry

    lax.fori_loop(0, 4 * units, step, 0)
    finish(last, low_b, sums_b, acc_b)
    merge_send(5, units - 1, T3, (IN34, IN35), IN03, zp)

    for u in range(units):
        merge_send(6, u, T1, (IN16,), IN01, bwd)

    def a_copy(number, u, place_from, place_to, to):
        k = place_to * units + u
        return remote(
            abuf.at[place_from * units + u], abuf.at[k], a_send.at[number * units + u], a_recv.at[k], to
        )

    def a_relay1(u):
        wait_in(abuf, a_recv, T1 * units + u)
        a_copy(3, u, T1, T6, fwd).start()
        wait_in(abuf, a_recv, T3 * units + u)
        a_copy(4, u, T3, T4, fwd).start()
        a_copy(5, u, T3, T5, bwd).start()

    def a_relay2(u):
        wait_in(abuf, a_recv, T6 * units + u)
        a_copy(6, u, T6, T7, zp).start()

    tile = tiles[me]
    limit = lengths[tile // 4, tile // 2 % 2] - tile % 2 * ROWS
    live = lax.broadcasted_iota(jnp.int32, (ROWS, UCOLS), 0) < limit
    for u in range(units):
        o, _ = merged(u, T0, (IN02, IN03, IN01))
        abuf[T0 * units + u] = jnp.where(live, o, 0.0).astype(jnp.bfloat16)
        a_copy(0, u, T0, T1, fwd).start()
        a_copy(1, u, T0, T2, bwd).start()
        a_copy(2, u, T0, T3, zp).start()

    def far_copy(zt, part, source):
        k = zt * 2 + part
        return remote(pbuf.at[source * 2 + part], far_in.at[k], far_send.at[k], far_recv.at[k], xbwd)

    def leaf_copy(zt, part, source):
        k = zt * 2 + part
        return remote(pbuf.at[source * 2 + part], leaf_in.at[k], leaf_send.at[k], leaf_recv.at[k], xfwd)

    def inter_copy(zt, part, source):
        k = zt * 2 + part
        return remote(pbuf.at[source * 2 + part], inter_in.at[k], inter_send.at[k], inter_recv.at[k], xbwd)

    def project(place):
        zf, steps = PLACES[place]
        home = seq(zf, steps) // 2
        rows = jnp.concatenate([abuf[place * units + u] for u in range(units)], axis=1)
        for part in range(2):
            pbuf[home * 2 + part] = jnp.dot(rows, wbuf[part], preferred_element_type=jnp.float32).astype(
                jnp.bfloat16
            )
        gap = (home // 2 - x + 4) % 4

        @pl.when(gap == 2)
        def _():
            for part in range(2):
                far_copy(home % 2, part, home).start()

        @pl.when(gap == (d + 4) % 4)
        def _():
            for part in range(2):
                leaf_copy(home % 2, part, home).start()

    def settle(place):
        for u in range(units):
            wait_in(abuf, a_recv, place * units + u)

    wload.wait()
    wsend.wait_recv()
    project(T0)
    for u in range(units):
        a_relay1(u)
    project(T1)
    project(T3)
    settle(T2)
    project(T2)
    for u in range(units):
        a_relay2(u)
    project(T6)
    settle(T5)
    project(T5)
    settle(T4)
    project(T4)
    settle(T7)
    project(T7)

    f32 = jnp.float32
    inter_home = (x - d + 4) % 4 * 2
    for zt in (1 - zh, zh):
        for part in range(2):
            k, m = zt * 2 + part, (inter_home + zt) * 2 + part
            wait_in(far_in, far_recv, k)
            pbuf[m] = (pbuf[m].astype(f32) + far_in[k].astype(f32)).astype(jnp.bfloat16)
            inter_copy(zt, part, inter_home + zt).start()

    def column_sum(zt, part):
        k = zt * 2 + part
        wait_in(leaf_in, leaf_recv, k)
        wait_in(inter_in, inter_recv, k)
        here = pbuf[(x * 2 + zt) * 2 + part].astype(f32)
        return here + leaf_in[k].astype(f32) + inter_in[k].astype(f32)

    def z_copy(part):
        return remote(zout.at[part], zin.at[part], z_send.at[part], z_recv.at[part], zhp)

    for part in range(2):
        zout[part] = column_sum(1 - zh, part).astype(jnp.bfloat16)
        z_copy(part).start()
    for part in range(2):
        fin[part] = column_sum(zh, part)
    for part in range(2):
        wait_in(zin, z_recv, part)
    xout[...] = (fin[1 - c] + zin[1 - c].astype(f32)).astype(jnp.bfloat16)
    last_copy = remote(xout, out.at[c], x_sem.at[0], x_sem.at[1], other)
    last_copy.start()
    out[c] = (fin[c] + zin[c].astype(f32)).astype(jnp.bfloat16)
    last_copy.wait()

    for copy in sends0 + kvs + [wsend]:
        copy.wait_send()
    for part in range(2):
        z_copy(part).wait_send()
        for zt in range(2):
            far_copy(zt, part, 0).wait_send()
            leaf_copy(zt, part, 0).wait_send()
            inter_copy(zt, part, 0).wait_send()

    def drain(u, carry):
        for make in (q_copy, a_copy):
            for number, src, dst, to in ((3, T1, T6, fwd), (4, T3, T4, fwd), (5, T3, T5, bwd), (6, T6, T7, zp)):
                make(number, u, src, dst, to).wait_send()
        for number, dst, to in ((0, T1, fwd), (1, T2, bwd), (2, T3, zp)):
            a_copy(number, u, T0, dst, to).wait_send()
        for number, place, slot, to in (
            (0, T2, IN02, fwd), (1, T5, IN35, fwd), (2, T7, IN67, zp), (3, T4, IN34, bwd),
            (4, T6, IN16, bwd), (5, T3, IN03, zp), (6, T1, IN01, bwd),
        ):
            for copy in o_copy(number, u, place, slot, to):
                copy.wait_send()
        return carry

    lax.fori_loop(0, units, drain, 0)


def attend(lengths, prompts, tiles, q, ck, cv, pk, pv, weight):
    units = q.shape[2] // UCOLS
    kd = pk.shape[1]
    cols = weight.shape[1]
    keys = 2 * kd + 2 * ROWS
    bf, f32 = jnp.bfloat16, jnp.float32
    smem = pl.BlockSpec(memory_space=pltpu.SMEM)
    hbm = pl.BlockSpec(memory_space=pl.ANY)
    dma = pltpu.SemaphoreType.DMA
    return pl.pallas_call(
        functools.partial(attend_kernel, units),
        out_shape=jax.ShapeDtypeStruct((2, ROWS, weight.shape[1]), bf),
        in_specs=[smem] * 3 + [hbm] * 6,
        out_specs=pl.BlockSpec(memory_space=pltpu.VMEM),
        scratch_shapes=[
            pltpu.VMEM((2, 2 * kd, WIDTH), bf),
            pltpu.VMEM((2, 2 * kd, WIDTH), bf),
            pltpu.VMEM((2 * ROWS, WIDTH), bf),
            pltpu.VMEM((2 * ROWS, WIDTH), bf),
            pltpu.VMEM((8 * units, ROWS, UCOLS), bf),
            pltpu.VMEM((8 * units, ROWS, UCOLS), bf),
            pltpu.VMEM((7 * units, ROWS, UCOLS), bf),
            pltpu.VMEM((8 * units, 8, ROWS), f32),
            pltpu.VMEM((7 * units, 8, ROWS), f32),
            pltpu.VMEM((UROWS, keys), f32),
            pltpu.VMEM((UROWS, keys), f32),
            pltpu.VMEM((UROWS, 128), f32),
            pltpu.VMEM((UROWS, 128), f32),
            pltpu.VMEM((UROWS, 128), f32),
            pltpu.VMEM((UROWS, 128), f32),
            pltpu.VMEM((UROWS, 128), f32),
            pltpu.VMEM((UROWS, 128), f32),
            pltpu.VMEM((UROWS, 128), f32),
            pltpu.VMEM((UROWS, 128), f32),
            pltpu.SMEM((8, 4), jnp.int32),
            pltpu.VMEM((2,) + weight.shape, bf),
            pltpu.VMEM((8 * units, ROWS, UCOLS), bf),
            pltpu.VMEM((16, ROWS, cols), bf),
            pltpu.VMEM((4, ROWS, cols), bf),
            pltpu.VMEM((4, ROWS, cols), bf),
            pltpu.VMEM((4, ROWS, cols), bf),
            pltpu.VMEM((2, ROWS, cols), bf),
            pltpu.VMEM((2, ROWS, cols), bf),
            pltpu.VMEM((2, ROWS, cols), f32),
            pltpu.VMEM((ROWS, cols), bf),
            dma((5 + units,)),
            dma((5,)),
            dma((5,)),
            dma((7 * units,)),
            dma((8 * units,)),
            dma((7 * units,)),
            dma((7 * units,)),
            dma((7 * units,)),
            dma((7 * units,)),
            dma((7 * units,)),
            dma((8 * units,)),
            dma((4,)),
            dma((4,)),
            dma((4,)),
            dma((4,)),
            dma((4,)),
            dma((4,)),
            dma((2,)),
            dma((2,)),
            dma((2,)),
        ],
        compiler_params=pltpu.CompilerParams(
            collective_id=0, has_side_effects=True, vmem_limit_bytes=60 << 20
        ),
        name="attend",
    )(lengths, prompts, tiles, q, ck, cv, pk, pv, weight)


def local(q, ck, cv, pk, pv, lengths, prompts, tiles, weight):
    return attend(lengths, prompts, tiles, q, ck, cv, pk, pv, weight)


def solution(mesh):
    return jax.shard_map(
        local,
        mesh=mesh,
        in_specs=(
            P("seq", None, "head"),
            P("seq", None, "head"),
            P("seq", None, "head"),
            P(None, "seq", "head"),
            P(None, "seq", "head"),
            P(),
            P(),
            P(),
            P("head", "seq"),
        ),
        out_specs=P("head", None, "seq"),
        check_vma=False,
    )
```

```python
import functools
import math

import jax
import jax.numpy as jnp
from jax import lax
from jax.experimental import pallas as pl
from jax.experimental.pallas import tpu as pltpu
from jax.sharding import PartitionSpec as P

QUERY_HEADS = 64
KEY_VALUE_HEADS = 8
WIDTH = 128
ROWS = 128
VERY_LOW = -1e30
SCALE = math.log2(math.e) / math.sqrt(WIDTH)
MESH = pl.DeviceIdType.MESH

HEADS_UNIT = 2
UCOLS = HEADS_UNIT * WIDTH
UROWS = HEADS_UNIT * ROWS
CHUNK = 512
RELAYS1 = ((1, (0,)), (2, (1,)), (3, (2,)), (4, (3,)))
RELAYS2 = ((5, (0, 1)), (6, (2,)), (7, (3,)))

PLACES = ((0, 0), (0, 3), (1, 0), (1, 1), (1, 2), (1, 3), (0, 2), (0, 1))
T0, T1, T3, T5, T7, T4, T6, T2 = range(8)


def at(place, u, units):
    if place in (T1, T3):
        return units + 2 * u + place - T1
    return place * units + u


IN67, IN16, IN34, IN35, IN01, IN02, IN03 = range(7)


def across(lhs, rhs):
    return lax.dot_general(lhs, rhs, (((1,), (1,)), ((), ())), preferred_element_type=jnp.float32)


def attend_kernel(
    units,
    lengths, prompts, tiles, q, ck, cv, pk, pv, weight,
    out,
    kall, vall, ckb, cvb, qbuf, obuf, rbuf, lob, lrb, sa, sb, ma, mb, low_a, low_b, sums_a, sums_b, acc_a, acc_b, info,
    wbuf, abuf, pbuf, far_in, leaf_in, inter_in, zin, zout, fin, xout,
    load_sem, kv_send, kv_recv, q_send, q_recv, o_send, o_recv, l_send, l_recv,
    a_send, a_recv, far_recv, leaf_recv, inter_recv, z_recv, f_send, x_sem,
):
    me = lax.axis_index("seq")
    z, y, c = me // 8, (me // 2) % 4, me % 2
    d = 1 - 2 * c
    kd = pk.shape[1]

    def seq(zf, steps):
        return (z + zf) % 2 * 8 + (y + steps * d + 8) % 4 * 2 + c

    def dev(zf, steps):
        return {"seq": seq(zf, steps)}

    other = {"seq": me + d}
    zp, fwd, bwd = dev(1, 0), dev(0, 1), dev(0, -1)
    group = lax.axis_index("head")
    x, zh = group // 2, group % 2
    xfwd = {"head": (x + d + 4) % 4 * 2 + zh}
    xbwd = {"head": (x - d + 4) % 4 * 2 + zh}
    zhp = {"head": x * 2 + 1 - zh}

    loads = [
        pltpu.make_async_copy(pk, kall.at[:, pl.ds(0, kd), :], load_sem.at[0]),
        pltpu.make_async_copy(pv, vall.at[:, pl.ds(0, kd), :], load_sem.at[1]),
        pltpu.make_async_copy(ck.at[0], ckb.at[pl.ds(0, ROWS), :], load_sem.at[2]),
        pltpu.make_async_copy(cv.at[0], cvb.at[pl.ds(0, ROWS), :], load_sem.at[3]),
    ] + [
        pltpu.make_async_copy(q.at[0, :, pl.ds(u * UCOLS, UCOLS)], qbuf.at[u], load_sem.at[4 + u])
        for u in range(units)
    ]
    wload = pltpu.make_async_copy(weight, wbuf.at[c], load_sem.at[4 + units])
    for copy in loads:
        copy.start()

    barrier = pltpu.get_barrier_semaphore()
    for peer in (other, zp, fwd, bwd, xfwd, xbwd, zhp):
        pl.semaphore_signal(barrier, inc=1, device_id=peer, device_id_type=MESH)
    pl.semaphore_wait(barrier, 7)

    last = 8 * units - 1

    def remote(src, dst, send, recv, to):
        return pltpu.make_async_remote_copy(
            src_ref=src, dst_ref=dst, send_sem=send, recv_sem=recv, device_id=to, device_id_type=MESH
        )

    def kv_copies():
        return [
            remote(pk, kall.at[:, pl.ds(kd, kd), :], kv_send.at[0], kv_recv.at[0], other),
            remote(ck.at[0], ckb.at[pl.ds(ROWS, ROWS), :], kv_send.at[2], kv_recv.at[2], other),
            remote(pv, vall.at[:, pl.ds(kd, kd), :], kv_send.at[1], kv_recv.at[1], other),
            remote(cv.at[0], cvb.at[pl.ds(ROWS, ROWS), :], kv_send.at[3], kv_recv.at[3], other),
        ]

    wsend = remote(weight, wbuf.at[c], kv_send.at[4], kv_recv.at[4], other)

    def q_copy(number, u, place_from, place_to, to):
        src = q.at[0, :, pl.ds(u * UCOLS, UCOLS)] if place_from is None else qbuf.at[at(place_from, u, units)]
        k = at(place_to, u, units)
        return remote(src, qbuf.at[k], q_send.at[0], q_recv.at[k], to)

    sends0 = []
    for u in range(units):
        sends0 += [
            q_copy(0, u, None, T1, fwd),
            q_copy(1, u, None, T2, bwd),
            q_copy(2, u, None, T3, zp),
        ]
    kvs = kv_copies()
    for copy in sends0[:3]:
        copy.start()
    for copy in kvs:
        copy.start()
    for copy in sends0[3:]:
        copy.start()

    mine, theirs = tiles[me], tiles[me + d]
    for place, (zf, steps) in enumerate(PLACES):
        tile = tiles[seq(zf, steps)]
        info[place, 0] = prompts[tile // 4]
        for k, held in enumerate((mine, theirs)):
            gap = (tile % 2 - held % 2) * ROWS
            info[place, 1 + k] = jnp.where(tile // 2 == held // 2, gap, -4 * ROWS)

    ahead = lax.broadcasted_iota(jnp.int32, (UROWS, ROWS), 1) - (
        lax.broadcasted_iota(jnp.int32, (UROWS, ROWS), 0) % ROWS
    )

    def wait_in(buf, sems, k):
        pltpu.make_async_copy(buf.at[k], buf.at[k], sems.at[k]).wait()

    def o_copy(number, u, place, slot, to):
        k, j = at(place, u, units), slot * units + u
        return (
            remote(obuf.at[k], rbuf.at[j], o_send.at[0], o_recv.at[j], to),
            remote(lob.at[k], lrb.at[j], l_send.at[0], l_recv.at[j], to),
        )

    def send_out(number, u, place, slot, to):
        for copy in o_copy(number, u, place, slot, to):
            copy.start()

    def merged(u, place, slots):
        k = at(place, u, units)
        js = [slot * units + u for slot in slots]
        for j in js:
            wait_in(rbuf, o_recv, j)
            wait_in(lrb, l_recv, j)
        logs = [lob[k]] + [lrb[j] for j in js]
        peak = functools.reduce(jnp.maximum, logs)
        weights = [jnp.exp2(x - peak) for x in logs]
        total = functools.reduce(jnp.add, weights)
        values = [obuf[k]] + [rbuf[j] for j in js]
        parts = []
        for head in range(HEADS_UNIT):
            acc = None
            for w, v in zip(weights, values):
                share = (w / total)[head : head + 1, :]
                column = jnp.broadcast_to(share, (ROWS, ROWS)).T
                term = column * v[:, head * WIDTH : (head + 1) * WIDTH].astype(jnp.float32)
                acc = term if acc is None else acc + term
            parts.append(acc)
        return jnp.concatenate(parts, axis=1), peak + jnp.log2(total)

    def merge_send(number, u, place, slots, slot, to):
        o, log = merged(u, place, slots)
        obuf[at(place, u, units)] = o.astype(jnp.bfloat16)
        lob[at(place, u, units)] = log
        send_out(number, u, place, slot, to)

    def relay1(u):
        wait_in(qbuf, q_recv, at(T1, u, units))
        q_copy(3, u, T1, T6, fwd).start()
        wait_in(qbuf, q_recv, at(T3, u, units))
        q_copy(4, u, T3, T4, fwd).start()
        q_copy(5, u, T3, T5, bwd).start()

    def relay2(u):
        wait_in(qbuf, q_recv, at(T6, u, units))
        q_copy(6, u, T6, T7, zp).start()

    def before(k):
        for relays, relay in ((RELAYS1, relay1), (RELAYS2, relay2)):
            for block, passed in relays:

                @pl.when(k == block)
                def _():
                    for u in passed:
                        relay(u)

        for ahead_by in (1, 2):
            n = 2 * k + ahead_by

            @pl.when(((n >= T5 * units) & (n < T6 * units)) | ((n >= T2 * units) & (n <= last)))
            def _():
                wait_in(qbuf, q_recv, n)

    def after(n):
        def at_unit(first, action):
            @pl.when((n >= first) & (n < first + units))
            def _():
                action(n - first)

        at_unit(T5 * units, lambda u: send_out(1, u, T5, IN35, fwd))
        at_unit(T7 * units, lambda u: send_out(2, u, T7, IN67, zp))
        at_unit(T4 * units, lambda u: send_out(3, u, T4, IN34, bwd))
        at_unit(T6 * units, lambda u: merge_send(4, u, T6, (IN67,), IN16, bwd))
        at_unit(T6 * units + 2, lambda u: merge_send(5, u, T3, (IN34, IN35), IN03, zp))
        at_unit(T2 * units, lambda u: send_out(0, u, T2, IN02, fwd))
        at_unit(T2 * units + 1, lambda u: merge_send(6, u, T1, (IN16,), IN01, bwd))

    chunks = [(i * CHUNK, CHUNK) for i in range(2 * kd // CHUNK)]
    total_keys = 2 * kd

    def fold(op, x):
        parts = [x[:, i : i + 128] for i in range(0, x.shape[1], 128)]
        return functools.reduce(op, parts)

    def place_of(n):
        n = jnp.int32(n)
        return jnp.where((n >= units) & (n < 3 * units), T1 + (n - units) % 2, n // units)

    def both(n1, s1, m1, n2, s2, m2, low2, sums2, acc2):
        first = n1 is not None
        second = n2 is not None
        if first:
            place1 = place_of(n1)
            p1 = info[place1, 0]
            raw = qbuf[n1]
            query = jnp.concatenate([raw[:, i * WIDTH : (i + 1) * WIDTH] for i in range(HEADS_UNIT)], axis=0)
            peak = None
        if second:
            p2 = info[place_of(n2), 0]
            low = jnp.broadcast_to(jnp.max(m2[...], axis=1, keepdims=True) * SCALE, (UROWS, 128))
            sums = jnp.zeros((UROWS, 128), jnp.float32)
            acc = jnp.zeros((UROWS, WIDTH), jnp.float32)
        for at, size in chunks + [(total_keys, 2 * ROWS)]:
            own = at >= total_keys
            if first:
                keys = ckb[...] if own else kall[p1, pl.ds(at, size), :]
                s = across(query, keys)
                if own:
                    s = jnp.concatenate(
                        [
                            jnp.where(ahead <= info[place1, 1 + k], s[:, k * ROWS : (k + 1) * ROWS], VERY_LOW)
                            for k in range(2)
                        ],
                        axis=1,
                    )
                s1[:, pl.ds(at, size)] = s
                top = fold(jnp.maximum, s)
                peak = top if peak is None else jnp.maximum(peak, top)
            if second:
                rows = cvb[...] if own else vall[p2, pl.ds(at, size), :]
                w = jnp.exp2(s2[:, pl.ds(at, size)] * SCALE - jnp.concatenate([low] * (size // 128), axis=1))
                sums = sums + fold(jnp.add, w)
                acc = acc + jnp.dot(w.astype(jnp.bfloat16), rows, preferred_element_type=jnp.float32)
        if first:
            m1[...] = peak
        if second:
            low2[...] = low
            sums2[...] = sums
            acc2[...] = acc

    def finish(n, low2, sums2, acc2):
        total = jnp.sum(sums2[...], axis=1, keepdims=True)
        o = acc2[...] / total
        log = low2[...] + jnp.log2(total)
        for i in range(HEADS_UNIT):
            obuf[n, :, i * WIDTH : (i + 1) * WIDTH] = o[i * ROWS : (i + 1) * ROWS].astype(jnp.bfloat16)
            lob[n, i : i + 1, :] = log[i * ROWS : (i + 1) * ROWS].T[0:1, :]

    lob[...] = jnp.zeros_like(lob)
    sums_b[...] = jnp.ones_like(sums_b)
    for n in (0, 2, 4):
        loads[n].wait()
    kvs[0].wait_recv()
    kvs[1].wait_recv()
    both(0, sa, ma, None, None, None, None, None, None)
    for n in (1, 3) + tuple(range(5, 4 + units)):
        loads[n].wait()
    kvs[2].wait_recv()
    kvs[3].wait_recv()
    wload.start()
    wsend.start()

    def step(k, carry):
        n = 2 * k
        before(k)
        finish(jnp.maximum(n - 1, 0), low_b, sums_b, acc_b)
        both(n + 1, sb, mb, n, sa, ma, low_a, sums_a, acc_a)
        finish(n, low_a, sums_a, acc_a)
        both(jnp.minimum(n + 2, last), sa, ma, n + 1, sb, mb, low_b, sums_b, acc_b)
        after(n - 1)
        after(n)
        return carry

    lax.fori_loop(0, 4 * units, step, 0)
    finish(last, low_b, sums_b, acc_b)
    send_out(0, units - 1, T2, IN02, fwd)
    merge_send(6, units - 2, T1, (IN16,), IN01, bwd)
    merge_send(6, units - 1, T1, (IN16,), IN01, bwd)

    def a_copy(number, u, place_from, place_to, to):
        k = place_to * units + u
        return remote(
            abuf.at[place_from * units + u], abuf.at[k], a_send.at[0], a_recv.at[k], to
        )

    def a_relay1(u):
        wait_in(abuf, a_recv, T1 * units + u)
        a_copy(3, u, T1, T6, fwd).start()
        wait_in(abuf, a_recv, T3 * units + u)
        a_copy(4, u, T3, T4, fwd).start()
        a_copy(5, u, T3, T5, bwd).start()

    def a_relay2(u):
        wait_in(abuf, a_recv, T6 * units + u)
        a_copy(6, u, T6, T7, zp).start()

    tile = tiles[me]
    limit = lengths[tile // 2 % 2, tile // 4] - tile % 2 * ROWS
    live = lax.broadcasted_iota(jnp.int32, (ROWS, UCOLS), 0) < limit
    for u in range(units):
        o, _ = merged(u, T0, (IN02, IN03, IN01))
        abuf[T0 * units + u] = jnp.where(live, o, 0.0).astype(jnp.bfloat16)
        a_copy(0, u, T0, T1, fwd).start()
        a_copy(1, u, T0, T2, bwd).start()
        a_copy(2, u, T0, T3, zp).start()

    def far_copy(zt, part, source):
        k = zt * 2 + part
        return remote(pbuf.at[source * 2 + part], far_in.at[k], f_send.at[0], far_recv.at[k], xbwd)

    def leaf_copy(zt, part, source):
        k = zt * 2 + part
        return remote(pbuf.at[source * 2 + part], leaf_in.at[k], f_send.at[0], leaf_recv.at[k], xfwd)

    def inter_copy(zt, part, source):
        k = zt * 2 + part
        return remote(pbuf.at[source * 2 + part], inter_in.at[k], f_send.at[0], inter_recv.at[k], xbwd)

    def project(place):
        zf, steps = PLACES[place]
        home = seq(zf, steps) // 2
        rows = jnp.concatenate([abuf[place * units + u] for u in range(units)], axis=1)
        for part in range(2):
            pbuf[home * 2 + part] = jnp.dot(rows, wbuf[part], preferred_element_type=jnp.float32).astype(
                jnp.bfloat16
            )
        gap = (home // 2 - x + 4) % 4

        @pl.when(gap == 2)
        def _():
            for part in range(2):
                far_copy(home % 2, part, home).start()

        @pl.when(gap == (d + 4) % 4)
        def _():
            for part in range(2):
                leaf_copy(home % 2, part, home).start()

    def settle(place):
        for u in range(units):
            wait_in(abuf, a_recv, place * units + u)

    f32 = jnp.float32

    def pass_on(place):
        zf, steps = PLACES[place]
        home = seq(zf, steps) // 2

        @pl.when((home // 2 - x + d + 4) % 4 == 0)
        def _():
            for part in range(2):
                k, m = home % 2 * 2 + part, home * 2 + part
                wait_in(far_in, far_recv, k)
                pbuf[m] = (pbuf[m].astype(f32) + far_in[k].astype(f32)).astype(jnp.bfloat16)
                inter_copy(home % 2, part, home).start()

    wload.wait()
    wsend.wait_recv()
    project(T0)
    for u in range(units):
        a_relay1(u)
    project(T1)
    project(T3)
    settle(T2)
    project(T2)
    pass_on(T0)
    for u in range(units):
        a_relay2(u)
    project(T6)
    pass_on(T1)
    pass_on(T3)
    settle(T5)
    project(T5)
    pass_on(T2)
    settle(T4)
    project(T4)
    pass_on(T6)
    settle(T7)
    project(T7)
    pass_on(T5)
    pass_on(T4)
    pass_on(T7)

    def column_sum(zt, part):
        k = zt * 2 + part
        wait_in(leaf_in, leaf_recv, k)
        wait_in(inter_in, inter_recv, k)
        here = pbuf[(x * 2 + zt) * 2 + part].astype(f32)
        return here + leaf_in[k].astype(f32) + inter_in[k].astype(f32)

    def z_copy(part):
        return remote(zout.at[part], zin.at[part], f_send.at[0], z_recv.at[part], zhp)

    for part in range(2):
        zout[part] = column_sum(1 - zh, part).astype(jnp.bfloat16)
        z_copy(part).start()
    for part in range(2):
        fin[part] = column_sum(zh, part)
    for part in range(2):
        wait_in(zin, z_recv, part)
    xout[...] = (fin[1 - c] + zin[1 - c].astype(f32)).astype(jnp.bfloat16)
    last_copy = remote(xout, out.at[c], x_sem.at[0], x_sem.at[1], other)
    last_copy.start()
    out[c] = (fin[c] + zin[c].astype(f32)).astype(jnp.bfloat16)
    last_copy.wait()

    for copy in kvs + [wsend]:
        copy.wait_send()
    for buf, sem in ((qbuf, q_send), (obuf, o_send), (lob, l_send), (abuf, a_send)):
        whole = buf.at[pl.ds(0, 7 * units)]
        pltpu.make_async_copy(whole, whole, sem.at[0]).wait()
    whole = pbuf.at[pl.ds(0, 14)]
    pltpu.make_async_copy(whole, whole, f_send.at[0]).wait()


def attend(lengths, prompts, tiles, q, ck, cv, pk, pv, weight):
    units = q.shape[2] // UCOLS
    kd = pk.shape[1]
    cols = weight.shape[1]
    keys = 2 * kd + 2 * ROWS
    bf, f32 = jnp.bfloat16, jnp.float32
    smem = pl.BlockSpec(memory_space=pltpu.SMEM)
    hbm = pl.BlockSpec(memory_space=pl.ANY)
    dma = pltpu.SemaphoreType.DMA
    return pl.pallas_call(
        functools.partial(attend_kernel, units),
        out_shape=jax.ShapeDtypeStruct((2, ROWS, weight.shape[1]), bf),
        in_specs=[smem] * 3 + [hbm] * 6,
        out_specs=pl.BlockSpec(memory_space=pltpu.VMEM),
        scratch_shapes=[
            pltpu.VMEM((2, 2 * kd, WIDTH), bf),
            pltpu.VMEM((2, 2 * kd, WIDTH), bf),
            pltpu.VMEM((2 * ROWS, WIDTH), bf),
            pltpu.VMEM((2 * ROWS, WIDTH), bf),
            pltpu.VMEM((8 * units, ROWS, UCOLS), bf),
            pltpu.VMEM((8 * units, ROWS, UCOLS), bf),
            pltpu.VMEM((7 * units, ROWS, UCOLS), bf),
            pltpu.VMEM((8 * units, 8, ROWS), f32),
            pltpu.VMEM((7 * units, 8, ROWS), f32),
            pltpu.VMEM((UROWS, keys), f32),
            pltpu.VMEM((UROWS, keys), f32),
            pltpu.VMEM((UROWS, 128), f32),
            pltpu.VMEM((UROWS, 128), f32),
            pltpu.VMEM((UROWS, 128), f32),
            pltpu.VMEM((UROWS, 128), f32),
            pltpu.VMEM((UROWS, 128), f32),
            pltpu.VMEM((UROWS, 128), f32),
            pltpu.VMEM((UROWS, 128), f32),
            pltpu.VMEM((UROWS, 128), f32),
            pltpu.SMEM((8, 4), jnp.int32),
            pltpu.VMEM((2,) + weight.shape, bf),
            pltpu.VMEM((8 * units, ROWS, UCOLS), bf),
            pltpu.VMEM((16, ROWS, cols), bf),
            pltpu.VMEM((4, ROWS, cols), bf),
            pltpu.VMEM((4, ROWS, cols), bf),
            pltpu.VMEM((4, ROWS, cols), bf),
            pltpu.VMEM((2, ROWS, cols), bf),
            pltpu.VMEM((2, ROWS, cols), bf),
            pltpu.VMEM((2, ROWS, cols), f32),
            pltpu.VMEM((ROWS, cols), bf),
            dma((5 + units,)),
            dma((5,)),
            dma((5,)),
            dma((1,)),
            dma((8 * units,)),
            dma((1,)),
            dma((7 * units,)),
            dma((1,)),
            dma((7 * units,)),
            dma((1,)),
            dma((8 * units,)),
            dma((4,)),
            dma((4,)),
            dma((4,)),
            dma((2,)),
            dma((1,)),
            dma((2,)),
        ],
        compiler_params=pltpu.CompilerParams(
            collective_id=0, has_side_effects=True, vmem_limit_bytes=60 << 20
        ),
        name="attend",
    )(lengths, prompts, tiles, q, ck, cv, pk, pv, weight)


def local(q, ck, cv, pk, pv, lengths, prompts, tiles, weight):
    return attend(lengths.T, prompts, tiles, q, ck, cv, pk, pv, weight)


def solution(mesh):
    return jax.shard_map(
        local,
        mesh=mesh,
        in_specs=(
            P("seq", None, "head"),
            P("seq", None, "head"),
            P("seq", None, "head"),
            P(None, "seq", "head"),
            P(None, "seq", "head"),
            P(),
            P(),
            P(),
            P("head", "seq"),
        ),
        out_specs=P("head", None, "seq"),
        check_vma=False,
    )
```

```python
import functools
import math

import jax
import jax.numpy as jnp
from jax import lax
from jax.experimental import pallas as pl
from jax.experimental.pallas import tpu as pltpu
from jax.sharding import PartitionSpec as P

QUERY_HEADS = 64
KEY_VALUE_HEADS = 8
WIDTH = 128
ROWS = 128
VERY_LOW = -1e30
SCALE = math.log2(math.e) / math.sqrt(WIDTH)
MESH = pl.DeviceIdType.MESH

HEADS_UNIT = 2
UCOLS = HEADS_UNIT * WIDTH
UROWS = HEADS_UNIT * ROWS
CHUNK = 512
PIECES = 4
PIECES = 4
RELAYS1 = ((1, (0,)), (2, (1,)), (3, (2,)), (4, (3,)))
RELAYS2 = ((4, (0,)), (5, (1,)), (6, (2,)), (7, (3,)))

PLACES = ((0, 0), (0, 1), (1, 0), (1, 1), (1, 3), (1, 2), (0, 2), (0, 3))
T0, T2, T3, T5, T4, T7, T6, T1 = range(8)
UNITS = 4
ORDER = (
    (T0, 0), (T0, 1), (T0, 2), (T2, 0), (T3, 0), (T2, 1), (T3, 1), (T1, 0),
    (T1, 1), (T5, 0), (T5, 1), (T4, 0), (T4, 1), (T7, 0), (T6, 0), (T7, 1),
    (T6, 1), (T7, 2), (T7, 3), (T4, 2), (T4, 3), (T6, 2), (T6, 3), (T5, 2),
    (T5, 3), (T1, 2), (T1, 3), (T3, 2), (T3, 3), (T2, 2), (T2, 3), (T0, 3),
)


def at(place, u, units):
    return ORDER.index((place, u))


IN67, IN16, IN34, IN35, IN01, IN02, IN03 = range(7)


def across(lhs, rhs):
    return lax.dot_general(lhs, rhs, (((1,), (1,)), ((), ())), preferred_element_type=jnp.float32)


def attend_kernel(
    units,
    lengths, prompts, tiles, q, ck, cv, pk, pv, weight,
    out,
    kall, vall, ckb, cvb, qbuf, obuf, rbuf, lob, lrb, sa, sb, ma, mb, low_a, low_b, sums_a, sums_b, acc_a, acc_b, info,
    wbuf, abuf, pbuf, far_in, leaf_in, inter_in, zin, zout, fin, xout,
    load_sem, kv_send, kv_recv, q_send, q_recv, o_send, o_recv, l_send, l_recv,
    a_send, a_recv, far_recv, leaf_recv, inter_recv, z_recv, f_send, x_send, x_recv,
):
    me = lax.axis_index("seq")
    z, y, c = me // 8, (me // 2) % 4, me % 2
    d = 1 - 2 * c
    kd = pk.shape[1]

    def seq(zf, steps):
        return (z + zf) % 2 * 8 + (y + steps * d + 8) % 4 * 2 + c

    def dev(zf, steps):
        return {"seq": seq(zf, steps)}

    other = {"seq": me + d}
    zp, fwd, bwd = dev(1, 0), dev(0, 1), dev(0, -1)
    group = lax.axis_index("head")
    x, zh = group // 2, group % 2
    xfwd = {"head": (x + d + 4) % 4 * 2 + zh}
    xbwd = {"head": (x - d + 4) % 4 * 2 + zh}
    zhp = {"head": x * 2 + 1 - zh}

    loads = [
        pltpu.make_async_copy(pk, kall.at[:, pl.ds(0, kd), :], load_sem.at[0]),
        pltpu.make_async_copy(pv, vall.at[:, pl.ds(0, kd), :], load_sem.at[1]),
        pltpu.make_async_copy(ck.at[0], ckb.at[pl.ds(0, ROWS), :], load_sem.at[2]),
        pltpu.make_async_copy(cv.at[0], cvb.at[pl.ds(0, ROWS), :], load_sem.at[3]),
    ] + [
        pltpu.make_async_copy(q.at[0, :, pl.ds(u * UCOLS, UCOLS)], qbuf.at[at(T0, u, units)], load_sem.at[4 + u])
        for u in range(units)
    ]
    wload = pltpu.make_async_copy(weight, wbuf.at[c], load_sem.at[4 + units])
    for copy in loads:
        copy.start()

    barrier = pltpu.get_barrier_semaphore()
    for peer in (other, zp, fwd, bwd, xfwd, xbwd, zhp):
        pl.semaphore_signal(barrier, inc=1, device_id=peer, device_id_type=MESH)
    pl.semaphore_wait(barrier, 7)

    last = 8 * units - 1

    def remote(src, dst, send, recv, to):
        return pltpu.make_async_remote_copy(
            src_ref=src, dst_ref=dst, send_sem=send, recv_sem=recv, device_id=to, device_id_type=MESH
        )

    def kv_copies():
        return [
            remote(pk, kall.at[:, pl.ds(kd, kd), :], kv_send.at[0], kv_recv.at[0], other),
            remote(ck.at[0], ckb.at[pl.ds(ROWS, ROWS), :], kv_send.at[2], kv_recv.at[2], other),
            remote(pv, vall.at[:, pl.ds(kd, kd), :], kv_send.at[1], kv_recv.at[1], other),
            remote(cv.at[0], cvb.at[pl.ds(ROWS, ROWS), :], kv_send.at[3], kv_recv.at[3], other),
        ]

    wsend = remote(weight, wbuf.at[c], kv_send.at[4], kv_recv.at[4], other)

    def q_copy(number, u, place_from, place_to, to):
        src = q.at[0, :, pl.ds(u * UCOLS, UCOLS)] if place_from is None else qbuf.at[at(place_from, u, units)]
        k = at(place_to, u, units)
        return remote(src, qbuf.at[k], q_send.at[0], q_recv.at[k], to)

    sends0 = []
    for u in range(units):
        sends0 += [
            q_copy(0, u, None, T1, fwd),
            q_copy(1, u, None, T2, bwd),
            q_copy(2, u, None, T3, zp),
        ]
    kvs = kv_copies()
    for copy in sends0[:3]:
        copy.start()
    for copy in kvs:
        copy.start()
    for copy in sends0[3:]:
        copy.start()

    mine, theirs = tiles[me], tiles[me + d]
    for place, (zf, steps) in enumerate(PLACES):
        tile = tiles[seq(zf, steps)]
        prompt = prompts[tile // 4]
        reach = [
            jnp.where(tile // 2 == held // 2, (tile % 2 - held % 2) * ROWS, -4 * ROWS) for held in (mine, theirs)
        ]
        for u in range(units):
            n = at(place, u, units)
            info[n, 0] = prompt
            info[n, 1] = reach[0]
            info[n, 2] = reach[1]

    ahead = lax.broadcasted_iota(jnp.int32, (UROWS, ROWS), 1) - (
        lax.broadcasted_iota(jnp.int32, (UROWS, ROWS), 0) % ROWS
    )

    def wait_in(buf, sems, k):
        pltpu.make_async_copy(buf.at[k], buf.at[k], sems.at[k]).wait()

    def o_copy(number, u, place, slot, to):
        k, j = at(place, u, units), slot * units + u
        return (
            remote(obuf.at[k], rbuf.at[j], o_send.at[0], o_recv.at[j], to),
            remote(lob.at[k], lrb.at[j], l_send.at[0], l_recv.at[j], to),
        )

    def send_out(number, u, place, slot, to):
        for copy in o_copy(number, u, place, slot, to):
            copy.start()

    def merged(u, place, slots):
        k = at(place, u, units)
        js = [slot * units + u for slot in slots]
        for j in js:
            wait_in(rbuf, o_recv, j)
            wait_in(lrb, l_recv, j)
        logs = [lob[k]] + [lrb[j] for j in js]
        peak = functools.reduce(jnp.maximum, logs)
        weights = [jnp.exp2(x - peak) for x in logs]
        total = functools.reduce(jnp.add, weights)
        values = [obuf[k]] + [rbuf[j] for j in js]
        parts = []
        for head in range(HEADS_UNIT):
            acc = None
            for w, v in zip(weights, values):
                share = (w / total)[head : head + 1, :]
                column = jnp.broadcast_to(share, (ROWS, ROWS)).T
                term = column * v[:, head * WIDTH : (head + 1) * WIDTH].astype(jnp.float32)
                acc = term if acc is None else acc + term
            parts.append(acc)
        return jnp.concatenate(parts, axis=1), peak + jnp.log2(total)

    def merge_send(number, u, place, slots, slot, to):
        o, log = merged(u, place, slots)
        obuf[at(place, u, units)] = o.astype(jnp.bfloat16)
        lob[at(place, u, units)] = log
        send_out(number, u, place, slot, to)

    def relay1(u):
        wait_in(qbuf, q_recv, at(T1, u, units))
        q_copy(3, u, T1, T6, fwd).start()
        wait_in(qbuf, q_recv, at(T3, u, units))
        q_copy(4, u, T3, T4, fwd).start()
        q_copy(5, u, T3, T5, bwd).start()

    def relay2(u):
        wait_in(qbuf, q_recv, at(T6, u, units))
        q_copy(6, u, T6, T7, zp).start()

    def run_at(k, table):
        def choose(blocks):
            if len(blocks) == 1:

                @pl.when(k == blocks[0])
                def _():
                    for action in table[blocks[0]]:
                        action()

            else:
                middle = len(blocks) // 2
                lax.cond(
                    k < blocks[middle], lambda: choose(blocks[:middle]), lambda: choose(blocks[middle:])
                )

        choose(sorted(table))

    ahead_of = {}
    for block, u in ((1, 0), (2, 1), (3, 2), (4, 3)):
        ahead_of.setdefault(block, []).append(functools.partial(relay1, u))
    for block, u in ((4, 0), (5, 1), (6, 2), (7, 3)):
        ahead_of.setdefault(block, []).append(functools.partial(relay2, u))
    for n, (place, u) in enumerate(ORDER):
        if place in (T2, T5, T4, T7):
            ahead_of.setdefault((n - 1) // 2, []).append(functools.partial(wait_in, qbuf, q_recv, n))

    def leaf_out(place, u):
        number, slot, to = {T2: (0, IN02, fwd), T5: (1, IN35, fwd), T7: (2, IN67, zp), T4: (3, IN34, bwd)}[place]
        send_out(number, u, place, slot, to)

    def merge_out(place, u):
        number, slots, slot, to = {
            T6: (4, (IN67,), IN16, bwd),
            T3: (5, (IN34, IN35), IN03, zp),
            T1: (6, (IN16,), IN01, bwd),
        }[place]
        merge_send(number, u, place, slots, slot, to)

    def a_copy(number, u, place_from, place_to, to):
        k = place_to * units + u
        return remote(
            abuf.at[place_from * units + u], abuf.at[k], a_send.at[0], a_recv.at[k], to
        )

    def a_relay1(u):
        wait_in(abuf, a_recv, T3 * units + u)
        a_copy(5, u, T3, T5, bwd).start()
        if u >= units // 2:
            a_copy(1, u, T0, T2, bwd).start()
        a_copy(4, u, T3, T4, fwd).start()
        wait_in(abuf, a_recv, T1 * units + u)
        a_copy(3, u, T1, T6, fwd).start()

    def a_relay2(u):
        wait_in(abuf, a_recv, T6 * units + u)
        a_copy(6, u, T6, T7, zp).start()

    tile = tiles[me]
    limit = lengths[tile // 2 % 2, tile // 4] - tile % 2 * ROWS
    live = lax.broadcasted_iota(jnp.int32, (ROWS, UCOLS), 0) < limit
    def own_attention(u):
        o, _ = merged(u, T0, (IN02, IN03, IN01))
        abuf[T0 * units + u] = jnp.where(live, o, 0.0).astype(jnp.bfloat16)
        a_copy(0, u, T0, T1, fwd).start()
        if u < units // 2:
            a_copy(1, u, T0, T2, bwd).start()
        a_copy(2, u, T0, T3, zp).start()

    done_after = {
        block: [functools.partial(action, *args) for action, *args in actions]
        for block, actions in {
            2: [(leaf_out, T2, 0)],
            3: [(leaf_out, T2, 1)],
            5: [(leaf_out, T5, 0), (leaf_out, T5, 1)],
            6: [(leaf_out, T4, 0), (leaf_out, T4, 1)],
            7: [(leaf_out, T7, 0)],
            8: [(leaf_out, T7, 1)],
            9: [(leaf_out, T7, 2), (leaf_out, T7, 3), (merge_out, T6, 0)],
            10: [(merge_out, T6, 1), (merge_out, T3, 0), (leaf_out, T4, 2), (leaf_out, T4, 3)],
            11: [(merge_out, T1, 0), (merge_out, T3, 1)],
            12: [(merge_out, T1, 1), (merge_out, T6, 2), (merge_out, T6, 3), (leaf_out, T5, 2), (leaf_out, T5, 3)],
            13: [(own_attention, 0)],
            14: [(own_attention, 1), (merge_out, T1, 2), (merge_out, T1, 3), (merge_out, T3, 2)],
            15: [(leaf_out, T2, 2), (leaf_out, T2, 3), (merge_out, T3, 3)],
        }.items()
    }
    for block, actions in ahead_of.items():
        done_after.setdefault(block - 1, []).extend(actions)

    chunks = [(i * CHUNK, CHUNK) for i in range(2 * kd // CHUNK)]
    total_keys = 2 * kd

    def fold(op, x):
        parts = [x[:, i : i + 128] for i in range(0, x.shape[1], 128)]
        return functools.reduce(op, parts)

    def both(n1, s1, m1, n2, s2, m2, low2, sums2, acc2):
        first = n1 is not None
        second = n2 is not None
        if first:
            p1 = info[n1, 0]
            raw = qbuf[n1]
            query = jnp.concatenate([raw[:, i * WIDTH : (i + 1) * WIDTH] for i in range(HEADS_UNIT)], axis=0)
            peak = None
        if second:
            p2 = info[n2, 0]
            low = jnp.broadcast_to(jnp.max(m2[...], axis=1, keepdims=True) * SCALE, (UROWS, 128))
            sums = jnp.zeros((UROWS, 128), jnp.float32)
            acc = jnp.zeros((UROWS, WIDTH), jnp.float32)
        for at, size in chunks + [(total_keys, 2 * ROWS)]:
            own = at >= total_keys
            if first:
                keys = ckb[...] if own else kall[p1, pl.ds(at, size), :]
                s = across(query, keys)
                if own:
                    s = jnp.concatenate(
                        [
                            jnp.where(ahead <= info[n1, 1 + k], s[:, k * ROWS : (k + 1) * ROWS], VERY_LOW)
                            for k in range(2)
                        ],
                        axis=1,
                    )
                s1[:, pl.ds(at, size)] = s
                top = fold(jnp.maximum, s)
                peak = top if peak is None else jnp.maximum(peak, top)
            if second:
                rows = cvb[...] if own else vall[p2, pl.ds(at, size), :]
                w = jnp.exp2(s2[:, pl.ds(at, size)] * SCALE - jnp.concatenate([low] * (size // 128), axis=1))
                sums = sums + fold(jnp.add, w)
                acc = acc + jnp.dot(w.astype(jnp.bfloat16), rows, preferred_element_type=jnp.float32)
        if first:
            m1[...] = peak
        if second:
            low2[...] = low
            sums2[...] = sums
            acc2[...] = acc

    def finish(n, low2, sums2, acc2):
        total = jnp.sum(sums2[...], axis=1, keepdims=True)
        o = acc2[...] / total
        log = low2[...] + jnp.log2(total)
        for i in range(HEADS_UNIT):
            obuf[n, :, i * WIDTH : (i + 1) * WIDTH] = o[i * ROWS : (i + 1) * ROWS].astype(jnp.bfloat16)
            lob[n, i : i + 1, :] = log[i * ROWS : (i + 1) * ROWS].T[0:1, :]

    lob[...] = jnp.zeros_like(lob)
    sums_b[...] = jnp.ones_like(sums_b)
    for n in (0, 2, 4):
        loads[n].wait()
    kvs[0].wait_recv()
    kvs[1].wait_recv()
    both(0, sa, ma, None, None, None, None, None, None)
    for n in (1, 3) + tuple(range(5, 4 + units)):
        loads[n].wait()
    kvs[2].wait_recv()
    kvs[3].wait_recv()
    wload.start()
    wsend.start()

    def step(k, carry):
        n = 2 * k
        finish(jnp.maximum(n - 1, 0), low_b, sums_b, acc_b)
        both(n + 1, sb, mb, n, sa, ma, low_a, sums_a, acc_a)
        finish(n, low_a, sums_a, acc_a)
        both(jnp.minimum(n + 2, last), sa, ma, n + 1, sb, mb, low_b, sums_b, acc_b)
        run_at(k, done_after)
        return carry

    lax.fori_loop(0, 4 * units, step, 0)
    finish(last, low_b, sums_b, acc_b)

    a_relay1(0)
    a_relay1(1)
    own_attention(2)
    own_attention(3)

    f32 = jnp.float32
    half = ROWS // 2

    def piece_of(i):
        return (i + 2 * (1 - c)) % PIECES

    def x_copy(buf, sems, zt, piece, source, to):
        k = zt * PIECES + piece
        return remote(pbuf.at[source * PIECES + piece], buf.at[k], f_send.at[0], sems.at[k], to)

    def project(place):
        zf, steps = PLACES[place]
        home = seq(zf, steps) // 2
        rows = jnp.concatenate([abuf[place * units + u] for u in range(units)], axis=1)
        gap = (home // 2 - x + 4) % 4
        for part in range(2):
            r = jnp.dot(rows, wbuf[part], preferred_element_type=f32).astype(jnp.bfloat16)
            for i in range(2):
                pbuf[home * PIECES + part * 2 + i] = r[i * half : (i + 1) * half]
        for i in range(PIECES):
            piece = piece_of(i)

            @pl.when(gap == 2)
            def _():
                x_copy(far_in, far_recv, home % 2, piece, home, xbwd).start()

            @pl.when(gap == (d + 4) % 4)
            def _():
                x_copy(leaf_in, leaf_recv, home % 2, piece, home, xfwd).start()

    def settle(place):
        for u in range(units):
            wait_in(abuf, a_recv, place * units + u)

    def pass_on(place):
        zf, steps = PLACES[place]
        home = seq(zf, steps) // 2

        @pl.when((home // 2 - x + d + 4) % 4 == 0)
        def _():
            for i in range(PIECES):
                piece = piece_of(i)
                k, m = home % 2 * PIECES + piece, home * PIECES + piece
                wait_in(far_in, far_recv, k)
                pbuf[m] = (pbuf[m].astype(f32) + far_in[k].astype(f32)).astype(jnp.bfloat16)
                x_copy(inter_in, inter_recv, home % 2, piece, home, xbwd).start()

    wload.wait()
    wsend.wait_recv()
    project(T0)
    a_relay2(0)
    a_relay2(1)
    a_relay1(2)
    a_relay1(3)
    project(T3)
    project(T1)
    pass_on(T0)
    settle(T5)
    project(T5)
    settle(T2)
    project(T2)
    a_relay2(2)
    a_relay2(3)
    settle(T4)
    project(T4)
    project(T6)
    pass_on(T3)
    pass_on(T1)
    settle(T7)
    project(T7)
    pass_on(T5)
    pass_on(T2)
    pass_on(T4)
    pass_on(T6)
    pass_on(T7)

    def column_sum(zt, piece):
        k = zt * PIECES + piece
        wait_in(leaf_in, leaf_recv, k)
        wait_in(inter_in, inter_recv, k)
        here = pbuf[(x * 2 + zt) * PIECES + piece].astype(f32)
        return here + leaf_in[k].astype(f32) + inter_in[k].astype(f32)

    def z_copy(piece):
        return remote(zout.at[piece], zin.at[piece], f_send.at[0], z_recv.at[piece], zhp)

    for i in range(PIECES):
        piece = piece_of(i)
        zout[piece] = column_sum(1 - zh, piece).astype(jnp.bfloat16)
        z_copy(piece).start()
    for i in range(PIECES):
        piece = piece_of(i)
        fin[piece] = column_sum(zh, piece)
    last_copies = []
    for i in range(2):
        piece = (1 - c) * 2 + i
        wait_in(zin, z_recv, piece)
        xout[i] = (fin[piece] + zin[piece].astype(f32)).astype(jnp.bfloat16)
        rows = pl.ds(i * half, half)
        last_copies.append(remote(xout.at[i], out.at[c, rows], x_send.at[i], x_recv.at[i], other))
        last_copies[-1].start()
    for i in range(2):
        piece = c * 2 + i
        wait_in(zin, z_recv, piece)
        out[c, i * half : (i + 1) * half] = (fin[piece] + zin[piece].astype(f32)).astype(jnp.bfloat16)
    for copy in last_copies:
        copy.wait()

    for copy in kvs + [wsend]:
        copy.wait_send()
    for buf, sem in ((qbuf, q_send), (obuf, o_send), (lob, l_send), (abuf, a_send)):
        whole = buf.at[pl.ds(0, 7 * units)]
        pltpu.make_async_copy(whole, whole, sem.at[0]).wait()
    whole = pbuf.at[pl.ds(0, 7 * PIECES)]
    pltpu.make_async_copy(whole, whole, f_send.at[0]).wait()


def attend(lengths, prompts, tiles, q, ck, cv, pk, pv, weight):
    units = q.shape[2] // UCOLS
    assert units == UNITS
    kd = pk.shape[1]
    cols = weight.shape[1]
    keys = 2 * kd + 2 * ROWS
    bf, f32 = jnp.bfloat16, jnp.float32
    smem = pl.BlockSpec(memory_space=pltpu.SMEM)
    hbm = pl.BlockSpec(memory_space=pl.ANY)
    dma = pltpu.SemaphoreType.DMA
    return pl.pallas_call(
        functools.partial(attend_kernel, units),
        out_shape=jax.ShapeDtypeStruct((2, ROWS, weight.shape[1]), bf),
        in_specs=[smem] * 3 + [hbm] * 6,
        out_specs=pl.BlockSpec(memory_space=pltpu.VMEM),
        scratch_shapes=[
            pltpu.VMEM((2, 2 * kd, WIDTH), bf),
            pltpu.VMEM((2, 2 * kd, WIDTH), bf),
            pltpu.VMEM((2 * ROWS, WIDTH), bf),
            pltpu.VMEM((2 * ROWS, WIDTH), bf),
            pltpu.VMEM((8 * units, ROWS, UCOLS), bf),
            pltpu.VMEM((8 * units, ROWS, UCOLS), bf),
            pltpu.VMEM((7 * units, ROWS, UCOLS), bf),
            pltpu.VMEM((8 * units, 8, ROWS), f32),
            pltpu.VMEM((7 * units, 8, ROWS), f32),
            pltpu.VMEM((UROWS, keys), f32),
            pltpu.VMEM((UROWS, keys), f32),
            pltpu.VMEM((UROWS, 128), f32),
            pltpu.VMEM((UROWS, 128), f32),
            pltpu.VMEM((UROWS, 128), f32),
            pltpu.VMEM((UROWS, 128), f32),
            pltpu.VMEM((UROWS, 128), f32),
            pltpu.VMEM((UROWS, 128), f32),
            pltpu.VMEM((UROWS, 128), f32),
            pltpu.VMEM((UROWS, 128), f32),
            pltpu.SMEM((8 * units, 4), jnp.int32),
            pltpu.VMEM((2,) + weight.shape, bf),
            pltpu.VMEM((8 * units, ROWS, UCOLS), bf),
            pltpu.VMEM((8 * PIECES, ROWS // 2, cols), bf),
            pltpu.VMEM((2 * PIECES, ROWS // 2, cols), bf),
            pltpu.VMEM((2 * PIECES, ROWS // 2, cols), bf),
            pltpu.VMEM((2 * PIECES, ROWS // 2, cols), bf),
            pltpu.VMEM((PIECES, ROWS // 2, cols), bf),
            pltpu.VMEM((PIECES, ROWS // 2, cols), bf),
            pltpu.VMEM((PIECES, ROWS // 2, cols), f32),
            pltpu.VMEM((2, ROWS // 2, cols), bf),
            dma((5 + units,)),
            dma((5,)),
            dma((5,)),
            dma((1,)),
            dma((8 * units,)),
            dma((1,)),
            dma((7 * units,)),
            dma((1,)),
            dma((7 * units,)),
            dma((1,)),
            dma((8 * units,)),
            dma((2 * PIECES,)),
            dma((2 * PIECES,)),
            dma((2 * PIECES,)),
            dma((PIECES,)),
            dma((1,)),
            dma((2,)),
            dma((2,)),
        ],
        compiler_params=pltpu.CompilerParams(
            collective_id=0, has_side_effects=True, vmem_limit_bytes=60 << 20
        ),
        name="attend",
    )(lengths, prompts, tiles, q, ck, cv, pk, pv, weight)


def local(q, ck, cv, pk, pv, lengths, prompts, tiles, weight):
    return attend(lengths.T, prompts, tiles, q, ck, cv, pk, pv, weight)


def solution(mesh):
    return jax.shard_map(
        local,
        mesh=mesh,
        in_specs=(
            P("seq", None, "head"),
            P("seq", None, "head"),
            P("seq", None, "head"),
            P(None, "seq", "head"),
            P(None, "seq", "head"),
            P(),
            P(),
            P(),
            P("head", "seq"),
        ),
        out_specs=P("head", None, "seq"),
        check_vma=False,
    )
```

```python
import functools
import math

import jax
import jax.numpy as jnp
from jax import lax
from jax.experimental import pallas as pl
from jax.experimental.pallas import tpu as pltpu
from jax.sharding import PartitionSpec as P

QUERY_HEADS = 64
KEY_VALUE_HEADS = 8
WIDTH = 128
ROWS = 128
VERY_LOW = -1e30
SCALE = math.log2(math.e) / math.sqrt(WIDTH)
MESH = pl.DeviceIdType.MESH

HEADS_UNIT = 2
UCOLS = HEADS_UNIT * WIDTH
UROWS = HEADS_UNIT * ROWS
CHUNK = 256
PIECES = 4
PIECES = 4
RELAYS1 = ((1, (0,)), (2, (1,)), (3, (2,)), (4, (3,)))
RELAYS2 = ((4, (0,)), (5, (1,)), (6, (2,)), (7, (3,)))

PLACES = ((0, 0), (0, 1), (1, 0), (1, 1), (1, 3), (1, 2), (0, 2), (0, 3))
T0, T2, T3, T5, T4, T7, T6, T1 = range(8)
UNITS = 4
ORDER = (
    (T0, 0), (T0, 1), (T0, 2), (T2, 0), (T3, 0), (T2, 1), (T3, 1), (T1, 0),
    (T1, 1), (T5, 0), (T5, 1), (T4, 0), (T4, 1), (T7, 0), (T6, 0), (T7, 1),
    (T6, 1), (T4, 2), (T4, 3), (T7, 2), (T7, 3), (T6, 2), (T6, 3), (T5, 2),
    (T5, 3), (T1, 2), (T1, 3), (T3, 2), (T3, 3), (T2, 2), (T2, 3), (T0, 3),
)


def at(place, u, units):
    return ORDER.index((place, u))


IN67, IN16, IN34, IN35, IN01, IN02, IN03 = range(7)


def across(lhs, rhs):
    return lax.dot_general(lhs, rhs, (((1,), (1,)), ((), ())), preferred_element_type=jnp.float32)


def attend_kernel(
    units,
    lengths, prompts, tiles, q, ck, cv, pk, pv, weight,
    out,
    kall, vall, ckb, cvb, qbuf, obuf, rbuf, lob, lrb, sa, sb, ma, mb, low_a, low_b, sums_a, sums_b, acc_a, acc_b, info,
    wbuf, abuf, pbuf, far_in, leaf_in, inter_in, zin, zout, fin, xout,
    load_sem, kv_send, kv_recv, q_send, q_recv, o_send, o_recv, l_send, l_recv,
    a_send, a_recv, far_recv, leaf_recv, inter_recv, z_recv, f_send, x_send, x_recv,
):
    me = lax.axis_index("seq")
    z, y, c = me // 8, (me // 2) % 4, me % 2
    d = 1 - 2 * c
    kd = pk.shape[1]

    def seq(zf, steps):
        return (z + zf) % 2 * 8 + (y + steps * d + 8) % 4 * 2 + c

    def dev(zf, steps):
        return {"seq": seq(zf, steps)}

    other = {"seq": me + d}
    zp, fwd, bwd = dev(1, 0), dev(0, 1), dev(0, -1)
    group = lax.axis_index("head")
    x, zh = group // 2, group % 2
    xfwd = {"head": (x + d + 4) % 4 * 2 + zh}
    xbwd = {"head": (x - d + 4) % 4 * 2 + zh}
    zhp = {"head": x * 2 + 1 - zh}

    loads = [
        pltpu.make_async_copy(pk, kall.at[:, pl.ds(0, kd), :], load_sem.at[0]),
        pltpu.make_async_copy(pv, vall.at[:, pl.ds(0, kd), :], load_sem.at[1]),
        pltpu.make_async_copy(ck.at[0], ckb.at[pl.ds(0, ROWS), :], load_sem.at[2]),
        pltpu.make_async_copy(cv.at[0], cvb.at[pl.ds(0, ROWS), :], load_sem.at[3]),
    ] + [
        pltpu.make_async_copy(q.at[0, :, pl.ds(u * UCOLS, UCOLS)], qbuf.at[at(T0, u, units)], load_sem.at[4 + u])
        for u in range(units)
    ]
    wload = pltpu.make_async_copy(weight, wbuf.at[c], load_sem.at[4 + units])
    for copy in loads:
        copy.start()

    barrier = pltpu.get_barrier_semaphore()
    for peer in (other, zp, fwd, bwd, xfwd, xbwd, zhp):
        pl.semaphore_signal(barrier, inc=1, device_id=peer, device_id_type=MESH)
    pl.semaphore_wait(barrier, 7)

    last = 8 * units - 1

    def remote(src, dst, send, recv, to):
        return pltpu.make_async_remote_copy(
            src_ref=src, dst_ref=dst, send_sem=send, recv_sem=recv, device_id=to, device_id_type=MESH
        )

    def kv_copies():
        return [
            remote(pk, kall.at[:, pl.ds(kd, kd), :], kv_send.at[0], kv_recv.at[0], other),
            remote(ck.at[0], ckb.at[pl.ds(ROWS, ROWS), :], kv_send.at[2], kv_recv.at[2], other),
            remote(pv, vall.at[:, pl.ds(kd, kd), :], kv_send.at[1], kv_recv.at[1], other),
            remote(cv.at[0], cvb.at[pl.ds(ROWS, ROWS), :], kv_send.at[3], kv_recv.at[3], other),
        ]

    wsend = remote(weight, wbuf.at[c], kv_send.at[4], kv_recv.at[4], other)

    def q_copy(number, u, place_from, place_to, to):
        src = q.at[0, :, pl.ds(u * UCOLS, UCOLS)] if place_from is None else qbuf.at[at(place_from, u, units)]
        k = at(place_to, u, units)
        return remote(src, qbuf.at[k], q_send.at[0], q_recv.at[k], to)

    sends0 = []
    for u in range(units):
        sends0 += [
            q_copy(0, u, None, T1, fwd),
            q_copy(1, u, None, T2, bwd),
            q_copy(2, u, None, T3, zp),
        ]
    kvs = kv_copies()
    for copy in sends0[:3]:
        copy.start()
    for copy in kvs:
        copy.start()
    for copy in sends0[3:]:
        copy.start()

    mine, theirs = tiles[me], tiles[me + d]
    for place, (zf, steps) in enumerate(PLACES):
        tile = tiles[seq(zf, steps)]
        prompt = prompts[tile // 4]
        reach = [
            jnp.where(tile // 2 == held // 2, (tile % 2 - held % 2) * ROWS, -4 * ROWS) for held in (mine, theirs)
        ]
        for u in range(units):
            n = at(place, u, units)
            info[n, 0] = prompt
            info[n, 1] = reach[0]
            info[n, 2] = reach[1]

    ahead = lax.broadcasted_iota(jnp.int32, (UROWS, ROWS), 1) - (
        lax.broadcasted_iota(jnp.int32, (UROWS, ROWS), 0) % ROWS
    )

    def wait_in(buf, sems, k):
        pltpu.make_async_copy(buf.at[k], buf.at[k], sems.at[k]).wait()

    def o_copy(number, u, place, slot, to):
        k, j = at(place, u, units), slot * units + u
        return (
            remote(obuf.at[k], rbuf.at[j], o_send.at[0], o_recv.at[j], to),
            remote(lob.at[k], lrb.at[j], l_send.at[0], l_recv.at[j], to),
        )

    def send_out(number, u, place, slot, to):
        for copy in o_copy(number, u, place, slot, to):
            copy.start()

    def merged(u, place, slots):
        k = at(place, u, units)
        js = [slot * units + u for slot in slots]
        for j in js:
            wait_in(rbuf, o_recv, j)
            wait_in(lrb, l_recv, j)
        logs = [lob[k]] + [lrb[j] for j in js]
        peak = functools.reduce(jnp.maximum, logs)
        weights = [jnp.exp2(x - peak) for x in logs]
        total = functools.reduce(jnp.add, weights)
        values = [obuf[k]] + [rbuf[j] for j in js]
        parts = []
        for head in range(HEADS_UNIT):
            acc = None
            for w, v in zip(weights, values):
                share = (w / total)[head : head + 1, :]
                column = jnp.broadcast_to(share, (ROWS, ROWS)).T
                term = column * v[:, head * WIDTH : (head + 1) * WIDTH].astype(jnp.float32)
                acc = term if acc is None else acc + term
            parts.append(acc)
        return jnp.concatenate(parts, axis=1), peak + jnp.log2(total)

    def merge_send(number, u, place, slots, slot, to):
        o, log = merged(u, place, slots)
        obuf[at(place, u, units)] = o.astype(jnp.bfloat16)
        lob[at(place, u, units)] = log
        send_out(number, u, place, slot, to)

    def relay1(u):
        wait_in(qbuf, q_recv, at(T1, u, units))
        q_copy(3, u, T1, T6, fwd).start()
        wait_in(qbuf, q_recv, at(T3, u, units))
        q_copy(4, u, T3, T4, fwd).start()
        q_copy(5, u, T3, T5, bwd).start()

    def relay2(u):
        wait_in(qbuf, q_recv, at(T6, u, units))
        q_copy(6, u, T6, T7, zp).start()

    def run_at(k, table):
        def choose(blocks):
            if len(blocks) == 1:

                @pl.when(k == blocks[0])
                def _():
                    for action in table[blocks[0]]:
                        action()

            else:
                middle = len(blocks) // 2
                lax.cond(
                    k < blocks[middle], lambda: choose(blocks[:middle]), lambda: choose(blocks[middle:])
                )

        choose(sorted(table))

    ahead_of = {}
    for block, u in ((1, 0), (2, 1), (3, 2), (4, 3)):
        ahead_of.setdefault(block, []).append(functools.partial(relay1, u))
    for block, u in ((4, 0), (5, 1), (6, 2), (7, 3)):
        ahead_of.setdefault(block, []).append(functools.partial(relay2, u))
    for n, (place, u) in enumerate(ORDER):
        if place in (T2, T5, T4, T7):
            ahead_of.setdefault((n - 1) // 2, []).append(functools.partial(wait_in, qbuf, q_recv, n))

    def leaf_out(place, u):
        number, slot, to = {T2: (0, IN02, fwd), T5: (1, IN35, fwd), T7: (2, IN67, zp), T4: (3, IN34, bwd)}[place]
        send_out(number, u, place, slot, to)

    def merge_out(place, u):
        number, slots, slot, to = {
            T6: (4, (IN67,), IN16, bwd),
            T3: (5, (IN34, IN35), IN03, zp),
            T1: (6, (IN16,), IN01, bwd),
        }[place]
        merge_send(number, u, place, slots, slot, to)

    def a_copy(number, u, place_from, place_to, to):
        k = place_to * units + u
        return remote(
            abuf.at[place_from * units + u], abuf.at[k], a_send.at[0], a_recv.at[k], to
        )

    def a_relay1(u):
        wait_in(abuf, a_recv, T3 * units + u)
        a_copy(5, u, T3, T5, bwd).start()
        if u >= units // 2:
            a_copy(1, u, T0, T2, bwd).start()
        a_copy(4, u, T3, T4, fwd).start()
        wait_in(abuf, a_recv, T1 * units + u)
        a_copy(3, u, T1, T6, fwd).start()

    def a_relay2(u):
        wait_in(abuf, a_recv, T6 * units + u)
        a_copy(6, u, T6, T7, zp).start()

    tile = tiles[me]
    limit = lengths[tile // 2 % 2, tile // 4] - tile % 2 * ROWS
    live = lax.broadcasted_iota(jnp.int32, (ROWS, UCOLS), 0) < limit
    def own_attention(u):
        o, _ = merged(u, T0, (IN02, IN03, IN01))
        abuf[T0 * units + u] = jnp.where(live, o, 0.0).astype(jnp.bfloat16)
        a_copy(0, u, T0, T1, fwd).start()
        if u < units // 2:
            a_copy(1, u, T0, T2, bwd).start()
        a_copy(2, u, T0, T3, zp).start()

    done_after = {
        block: [functools.partial(action, *args) for action, *args in actions]
        for block, actions in {
            2: [(leaf_out, T2, 0)],
            3: [(leaf_out, T2, 1)],
            5: [(leaf_out, T5, 0), (leaf_out, T5, 1)],
            6: [(leaf_out, T4, 0), (leaf_out, T4, 1)],
            7: [(leaf_out, T7, 0)],
            8: [(leaf_out, T7, 1)],
            9: [(leaf_out, T4, 2), (leaf_out, T4, 3), (merge_out, T6, 0)],
            10: [(leaf_out, T7, 2), (leaf_out, T7, 3), (merge_out, T6, 1), (merge_out, T3, 0)],
            11: [(merge_out, T1, 0), (merge_out, T3, 1)],
            12: [(merge_out, T1, 1), (leaf_out, T5, 2), (leaf_out, T5, 3), (merge_out, T6, 2), (merge_out, T6, 3)],
            13: [(own_attention, 0)],
            14: [(merge_out, T3, 2), (own_attention, 1)],
            15: [(leaf_out, T2, 2), (leaf_out, T2, 3), (merge_out, T3, 3), (merge_out, T1, 2), (merge_out, T1, 3)],
        }.items()
    }
    for block, actions in ahead_of.items():
        done_after.setdefault(block - 1, []).extend(actions)

    chunks = [(i * CHUNK, CHUNK) for i in range(2 * kd // CHUNK)]
    total_keys = 2 * kd

    def fold(op, x):
        parts = [x[:, i : i + 128] for i in range(0, x.shape[1], 128)]
        return functools.reduce(op, parts)

    def both(n1, s1, m1, n2, s2, m2, low2, sums2, acc2):
        first = n1 is not None
        second = n2 is not None
        if first:
            p1 = info[n1, 0]
            raw = qbuf[n1]
            query = jnp.concatenate([raw[:, i * WIDTH : (i + 1) * WIDTH] for i in range(HEADS_UNIT)], axis=0)
            peak = None
        if second:
            p2 = info[n2, 0]
            low = jnp.broadcast_to(jnp.max(m2[...], axis=1, keepdims=True) * SCALE, (UROWS, 128))
            sums = jnp.zeros((UROWS, 128), jnp.float32)
            acc = jnp.zeros((UROWS, WIDTH), jnp.float32)
        for at, size in chunks + [(total_keys, 2 * ROWS)]:
            own = at >= total_keys
            if first:
                keys = ckb[...] if own else kall[p1, pl.ds(at, size), :]
                s = across(query, keys)
                if own:
                    s = jnp.concatenate(
                        [
                            jnp.where(ahead <= info[n1, 1 + k], s[:, k * ROWS : (k + 1) * ROWS], VERY_LOW)
                            for k in range(2)
                        ],
                        axis=1,
                    )
                s1[:, pl.ds(at, size)] = s
                top = fold(jnp.maximum, s)
                peak = top if peak is None else jnp.maximum(peak, top)
            if second:
                rows = cvb[...] if own else vall[p2, pl.ds(at, size), :]
                w = jnp.exp2(s2[:, pl.ds(at, size)] * SCALE - jnp.concatenate([low] * (size // 128), axis=1))
                sums = sums + fold(jnp.add, w)
                acc = acc + jnp.dot(w.astype(jnp.bfloat16), rows, preferred_element_type=jnp.float32)
        if first:
            m1[...] = peak
        if second:
            low2[...] = low
            sums2[...] = sums
            acc2[...] = acc

    def finish(n, low2, sums2, acc2):
        total = jnp.sum(sums2[...], axis=1, keepdims=True)
        o = acc2[...] / total
        log = low2[...] + jnp.log2(total)
        for i in range(HEADS_UNIT):
            obuf[n, :, i * WIDTH : (i + 1) * WIDTH] = o[i * ROWS : (i + 1) * ROWS].astype(jnp.bfloat16)
            lob[n, i : i + 1, :] = log[i * ROWS : (i + 1) * ROWS].T[0:1, :]

    lob[...] = jnp.zeros_like(lob)
    sums_b[...] = jnp.ones_like(sums_b)
    for n in (0, 2, 4):
        loads[n].wait()
    kvs[0].wait_recv()
    kvs[1].wait_recv()
    both(0, sa, ma, None, None, None, None, None, None)
    for n in (1, 3) + tuple(range(5, 4 + units)):
        loads[n].wait()
    kvs[2].wait_recv()
    kvs[3].wait_recv()
    wload.start()
    wsend.start()

    def step(k, carry):
        n = 2 * k
        finish(jnp.maximum(n - 1, 0), low_b, sums_b, acc_b)
        both(n + 1, sb, mb, n, sa, ma, low_a, sums_a, acc_a)
        finish(n, low_a, sums_a, acc_a)
        both(jnp.minimum(n + 2, last), sa, ma, n + 1, sb, mb, low_b, sums_b, acc_b)
        run_at(k, done_after)
        return carry

    lax.fori_loop(0, 4 * units, step, 0)
    finish(last, low_b, sums_b, acc_b)

    a_relay1(0)
    a_relay1(1)
    own_attention(2)
    own_attention(3)

    f32 = jnp.float32
    half = ROWS // 2

    def piece_of(i):
        return (i + 2 * (1 - c)) % PIECES

    def x_copy(buf, sems, zt, piece, source, to):
        k = zt * PIECES + piece
        return remote(pbuf.at[source * PIECES + piece], buf.at[k], f_send.at[0], sems.at[k], to)

    def project(place):
        zf, steps = PLACES[place]
        home = seq(zf, steps) // 2
        rows = jnp.concatenate([abuf[place * units + u] for u in range(units)], axis=1)
        gap = (home // 2 - x + 4) % 4
        for part in range(2):
            r = jnp.dot(rows, wbuf[part], preferred_element_type=f32).astype(jnp.bfloat16)
            for i in range(2):
                pbuf[home * PIECES + part * 2 + i] = r[i * half : (i + 1) * half]
        for i in range(PIECES):
            piece = piece_of(i)

            @pl.when(gap == 2)
            def _():
                x_copy(far_in, far_recv, home % 2, piece, home, xbwd).start()

            @pl.when(gap == (d + 4) % 4)
            def _():
                x_copy(leaf_in, leaf_recv, home % 2, piece, home, xfwd).start()

    def settle(place):
        for u in range(units):
            wait_in(abuf, a_recv, place * units + u)

    def pass_on(place):
        zf, steps = PLACES[place]
        home = seq(zf, steps) // 2

        @pl.when((home // 2 - x + d + 4) % 4 == 0)
        def _():
            for i in range(PIECES):
                piece = piece_of(i)
                k, m = home % 2 * PIECES + piece, home * PIECES + piece
                wait_in(far_in, far_recv, k)
                pbuf[m] = (pbuf[m].astype(f32) + far_in[k].astype(f32)).astype(jnp.bfloat16)
                x_copy(inter_in, inter_recv, home % 2, piece, home, xbwd).start()

    wload.wait()
    wsend.wait_recv()
    project(T0)
    a_relay2(0)
    a_relay2(1)
    a_relay1(2)
    a_relay1(3)
    project(T3)
    project(T1)
    pass_on(T0)
    settle(T5)
    project(T5)
    settle(T2)
    project(T2)
    a_relay2(2)
    a_relay2(3)
    settle(T4)
    project(T4)
    project(T6)
    pass_on(T3)
    pass_on(T1)
    settle(T7)
    project(T7)
    pass_on(T5)
    pass_on(T2)
    pass_on(T4)
    pass_on(T6)
    pass_on(T7)

    def column_sum(zt, piece):
        k = zt * PIECES + piece
        wait_in(leaf_in, leaf_recv, k)
        wait_in(inter_in, inter_recv, k)
        here = pbuf[(x * 2 + zt) * PIECES + piece].astype(f32)
        return here + leaf_in[k].astype(f32) + inter_in[k].astype(f32)

    def z_copy(piece):
        return remote(zout.at[piece], zin.at[piece], f_send.at[0], z_recv.at[piece], zhp)

    for i in range(PIECES):
        piece = piece_of(i)
        zout[piece] = column_sum(1 - zh, piece).astype(jnp.bfloat16)
        z_copy(piece).start()
    for i in range(PIECES):
        piece = piece_of(i)
        fin[piece] = column_sum(zh, piece)
    last_copies = []
    for i in range(2):
        piece = (1 - c) * 2 + i
        wait_in(zin, z_recv, piece)
        xout[i] = (fin[piece] + zin[piece].astype(f32)).astype(jnp.bfloat16)
        rows = pl.ds(i * half, half)
        last_copies.append(remote(xout.at[i], out.at[c, rows], x_send.at[i], x_recv.at[i], other))
        last_copies[-1].start()
    for i in range(2):
        piece = c * 2 + i
        wait_in(zin, z_recv, piece)
        out[c, i * half : (i + 1) * half] = (fin[piece] + zin[piece].astype(f32)).astype(jnp.bfloat16)
    for copy in last_copies:
        copy.wait()

    for copy in kvs + [wsend]:
        copy.wait_send()
    for buf, sem in ((qbuf, q_send), (obuf, o_send), (lob, l_send), (abuf, a_send)):
        whole = buf.at[pl.ds(0, 7 * units)]
        pltpu.make_async_copy(whole, whole, sem.at[0]).wait()
    whole = pbuf.at[pl.ds(0, 7 * PIECES)]
    pltpu.make_async_copy(whole, whole, f_send.at[0]).wait()


def attend(lengths, prompts, tiles, q, ck, cv, pk, pv, weight):
    units = q.shape[2] // UCOLS
    assert units == UNITS
    kd = pk.shape[1]
    cols = weight.shape[1]
    keys = 2 * kd + 2 * ROWS
    bf, f32 = jnp.bfloat16, jnp.float32
    smem = pl.BlockSpec(memory_space=pltpu.SMEM)
    hbm = pl.BlockSpec(memory_space=pl.ANY)
    dma = pltpu.SemaphoreType.DMA
    return pl.pallas_call(
        functools.partial(attend_kernel, units),
        out_shape=jax.ShapeDtypeStruct((2, ROWS, weight.shape[1]), bf),
        in_specs=[smem] * 3 + [hbm] * 6,
        out_specs=pl.BlockSpec(memory_space=pltpu.VMEM),
        scratch_shapes=[
            pltpu.VMEM((2, 2 * kd, WIDTH), bf),
            pltpu.VMEM((2, 2 * kd, WIDTH), bf),
            pltpu.VMEM((2 * ROWS, WIDTH), bf),
            pltpu.VMEM((2 * ROWS, WIDTH), bf),
            pltpu.VMEM((8 * units, ROWS, UCOLS), bf),
            pltpu.VMEM((8 * units, ROWS, UCOLS), bf),
            pltpu.VMEM((7 * units, ROWS, UCOLS), bf),
            pltpu.VMEM((8 * units, 8, ROWS), f32),
            pltpu.VMEM((7 * units, 8, ROWS), f32),
            pltpu.VMEM((UROWS, keys), f32),
            pltpu.VMEM((UROWS, keys), f32),
            pltpu.VMEM((UROWS, 128), f32),
            pltpu.VMEM((UROWS, 128), f32),
            pltpu.VMEM((UROWS, 128), f32),
            pltpu.VMEM((UROWS, 128), f32),
            pltpu.VMEM((UROWS, 128), f32),
            pltpu.VMEM((UROWS, 128), f32),
            pltpu.VMEM((UROWS, 128), f32),
            pltpu.VMEM((UROWS, 128), f32),
            pltpu.SMEM((8 * units, 4), jnp.int32),
            pltpu.VMEM((2,) + weight.shape, bf),
            pltpu.VMEM((8 * units, ROWS, UCOLS), bf),
            pltpu.VMEM((8 * PIECES, ROWS // 2, cols), bf),
            pltpu.VMEM((2 * PIECES, ROWS // 2, cols), bf),
            pltpu.VMEM((2 * PIECES, ROWS // 2, cols), bf),
            pltpu.VMEM((2 * PIECES, ROWS // 2, cols), bf),
            pltpu.VMEM((PIECES, ROWS // 2, cols), bf),
            pltpu.VMEM((PIECES, ROWS // 2, cols), bf),
            pltpu.VMEM((PIECES, ROWS // 2, cols), f32),
            pltpu.VMEM((2, ROWS // 2, cols), bf),
            dma((5 + units,)),
            dma((5,)),
            dma((5,)),
            dma((1,)),
            dma((8 * units,)),
            dma((1,)),
            dma((7 * units,)),
            dma((1,)),
            dma((7 * units,)),
            dma((1,)),
            dma((8 * units,)),
            dma((2 * PIECES,)),
            dma((2 * PIECES,)),
            dma((2 * PIECES,)),
            dma((PIECES,)),
            dma((1,)),
            dma((2,)),
            dma((2,)),
        ],
        compiler_params=pltpu.CompilerParams(
            collective_id=0, has_side_effects=True, vmem_limit_bytes=60 << 20
        ),
        name="attend",
    )(lengths, prompts, tiles, q, ck, cv, pk, pv, weight)


def local(q, ck, cv, pk, pv, lengths, prompts, tiles, weight):
    return attend(lengths.T, prompts, tiles, q, ck, cv, pk, pv, weight)


def solution(mesh):
    return jax.shard_map(
        local,
        mesh=mesh,
        in_specs=(
            P("seq", None, "head"),
            P("seq", None, "head"),
            P("seq", None, "head"),
            P(None, "seq", "head"),
            P(None, "seq", "head"),
            P(),
            P(),
            P(),
            P("head", "seq"),
        ),
        out_specs=P("head", None, "seq"),
        check_vma=False,
    )
```

```python
import functools
import math

import jax
import jax.numpy as jnp
from jax import lax
from jax.experimental import pallas as pl
from jax.experimental.pallas import tpu as pltpu
from jax.sharding import PartitionSpec as P

QUERY_HEADS = 64
KEY_VALUE_HEADS = 8
WIDTH = 128
ROWS = 128
VERY_LOW = -1e30
SCALE = math.log2(math.e) / math.sqrt(WIDTH)
MESH = pl.DeviceIdType.MESH

HEADS_UNIT = 2
UCOLS = HEADS_UNIT * WIDTH
UROWS = HEADS_UNIT * ROWS
CHUNK = 256
PIECES = 4
PIECES = 4
RELAYS1 = ((1, (0,)), (2, (1,)), (3, (2,)), (4, (3,)))
RELAYS2 = ((4, (0,)), (5, (1,)), (6, (2,)), (7, (3,)))

PLACES = ((0, 0), (0, 1), (1, 0), (1, 1), (1, 3), (1, 2), (0, 2), (0, 3))
T0, T2, T3, T5, T4, T7, T6, T1 = range(8)
UNITS = 4
ORDER = (
    (T0, 0), (T0, 1), (T0, 2), (T2, 0), (T3, 0), (T2, 1), (T3, 1), (T1, 0),
    (T1, 1), (T5, 0), (T5, 1), (T4, 0), (T4, 1), (T7, 0), (T6, 0), (T7, 1),
    (T6, 1), (T4, 2), (T4, 3), (T7, 2), (T7, 3), (T6, 2), (T6, 3), (T5, 2),
    (T5, 3), (T1, 2), (T1, 3), (T3, 2), (T3, 3), (T2, 2), (T2, 3), (T0, 3),
)


def at(place, u, units):
    return ORDER.index((place, u))


IN67, IN16, IN34, IN35, IN01, IN02, IN03 = range(7)


def across(lhs, rhs):
    return lax.dot_general(lhs, rhs, (((1,), (1,)), ((), ())), preferred_element_type=jnp.float32)


def attend_kernel(
    units,
    lengths, prompts, tiles, q, ck, cv, pk, pv, weight,
    out,
    kall, vall, ckb, cvb, qbuf, obuf, rbuf, lob, lrb, sa, sb, ma, mb, low_a, low_b, sums_a, sums_b, acc_a, acc_b, info,
    wbuf, abuf, pbuf, far_in, leaf_in, inter_in, zin, zout, fin, xout,
    load_sem, kv_send, kv_recv, q_send, q_recv, o_send, o_recv, l_send,
    a_send, a_recv, far_recv, leaf_recv, inter_recv, z_recv, f_send, x_send, x_recv,
):
    me = lax.axis_index("seq")
    z, y, c = me // 8, (me // 2) % 4, me % 2
    d = 1 - 2 * c
    kd = pk.shape[1]

    def seq(zf, steps):
        return (z + zf) % 2 * 8 + (y + steps * d + 8) % 4 * 2 + c

    def dev(zf, steps):
        return {"seq": seq(zf, steps)}

    other = {"seq": me + d}
    zp, fwd, bwd = dev(1, 0), dev(0, 1), dev(0, -1)
    group = lax.axis_index("head")
    x, zh = group // 2, group % 2
    xfwd = {"head": (x + d + 4) % 4 * 2 + zh}
    xbwd = {"head": (x - d + 4) % 4 * 2 + zh}
    zhp = {"head": x * 2 + 1 - zh}

    loads = [
        pltpu.make_async_copy(pk, kall.at[:, pl.ds(0, kd), :], load_sem.at[0]),
        pltpu.make_async_copy(pv, vall.at[:, pl.ds(0, kd), :], load_sem.at[1]),
        pltpu.make_async_copy(ck.at[0], ckb.at[pl.ds(0, ROWS), :], load_sem.at[2]),
        pltpu.make_async_copy(cv.at[0], cvb.at[pl.ds(0, ROWS), :], load_sem.at[3]),
    ] + [
        pltpu.make_async_copy(q.at[0, :, pl.ds(u * UCOLS, UCOLS)], qbuf.at[at(T0, u, units)], load_sem.at[4 + u])
        for u in range(units)
    ]
    wload = pltpu.make_async_copy(weight, wbuf.at[c], load_sem.at[4 + units])
    for copy in loads:
        copy.start()

    barrier = pltpu.get_barrier_semaphore()
    for peer in (other, zp, fwd, bwd, xfwd, xbwd, zhp):
        pl.semaphore_signal(barrier, inc=1, device_id=peer, device_id_type=MESH)
    pl.semaphore_wait(barrier, 7)

    last = 8 * units - 1

    def remote(src, dst, send, recv, to):
        return pltpu.make_async_remote_copy(
            src_ref=src, dst_ref=dst, send_sem=send, recv_sem=recv, device_id=to, device_id_type=MESH
        )

    def kv_copies():
        return [
            remote(pk, kall.at[:, pl.ds(kd, kd), :], kv_send.at[0], kv_recv.at[0], other),
            remote(ck.at[0], ckb.at[pl.ds(ROWS, ROWS), :], kv_send.at[2], kv_recv.at[2], other),
            remote(pv, vall.at[:, pl.ds(kd, kd), :], kv_send.at[1], kv_recv.at[1], other),
            remote(cv.at[0], cvb.at[pl.ds(ROWS, ROWS), :], kv_send.at[3], kv_recv.at[3], other),
        ]

    wsend = remote(weight, wbuf.at[c], kv_send.at[4], kv_recv.at[4], other)

    def q_copy(number, u, place_from, place_to, to):
        src = q.at[0, :, pl.ds(u * UCOLS, UCOLS)] if place_from is None else qbuf.at[at(place_from, u, units)]
        k = at(place_to, u, units)
        return remote(src, qbuf.at[k], q_send.at[0], q_recv.at[k], to)

    sends0 = []
    for u in range(units):
        sends0 += [
            q_copy(0, u, None, T1, fwd),
            q_copy(1, u, None, T2, bwd),
            q_copy(2, u, None, T3, zp),
        ]
    kvs = kv_copies()
    for copy in sends0[:3]:
        copy.start()
    for copy in kvs:
        copy.start()
    for copy in sends0[3:]:
        copy.start()

    mine, theirs = tiles[me], tiles[me + d]
    for place, (zf, steps) in enumerate(PLACES):
        tile = tiles[seq(zf, steps)]
        prompt = prompts[tile // 4]
        reach = [
            jnp.where(tile // 2 == held // 2, (tile % 2 - held % 2) * ROWS, -4 * ROWS) for held in (mine, theirs)
        ]
        for u in range(units):
            n = at(place, u, units)
            info[n, 0] = prompt
            info[n, 1] = reach[0]
            info[n, 2] = reach[1]

    ahead = lax.broadcasted_iota(jnp.int32, (UROWS, ROWS), 1) - (
        lax.broadcasted_iota(jnp.int32, (UROWS, ROWS), 0) % ROWS
    )

    def wait_in(buf, sems, k):
        pltpu.make_async_copy(buf.at[k], buf.at[k], sems.at[k]).wait()

    def o_copy(number, u, place, slot, to):
        k, j = at(place, u, units), slot * units + u
        return (
            remote(obuf.at[k], rbuf.at[j], o_send.at[0], o_recv.at[j], to),
            remote(lob.at[k], lrb.at[j], l_send.at[0], o_recv.at[j], to),
        )

    def send_out(number, u, place, slot, to):
        for copy in o_copy(number, u, place, slot, to):
            copy.start()

    def merged(u, place, slots):
        k = at(place, u, units)
        js = [slot * units + u for slot in slots]
        for j in js:
            both_bytes = lob.at[pl.ds(0, 17)]
            pltpu.make_async_copy(both_bytes, both_bytes, o_recv.at[j]).wait()
        logs = [lob[k]] + [lrb[j] for j in js]
        peak = functools.reduce(jnp.maximum, logs)
        weights = [jnp.exp2(x - peak) for x in logs]
        total = functools.reduce(jnp.add, weights)
        values = [obuf[k]] + [rbuf[j] for j in js]
        parts = []
        for head in range(HEADS_UNIT):
            acc = None
            for w, v in zip(weights, values):
                share = (w / total)[head : head + 1, :]
                column = jnp.broadcast_to(share, (ROWS, ROWS)).T
                term = column * v[:, head * WIDTH : (head + 1) * WIDTH].astype(jnp.float32)
                acc = term if acc is None else acc + term
            parts.append(acc)
        return jnp.concatenate(parts, axis=1), peak + jnp.log2(total)

    def merge_send(number, u, place, slots, slot, to):
        o, log = merged(u, place, slots)
        obuf[at(place, u, units)] = o.astype(jnp.bfloat16)
        lob[at(place, u, units)] = log
        send_out(number, u, place, slot, to)

    def relay1(u):
        wait_in(qbuf, q_recv, at(T1, u, units))
        q_copy(3, u, T1, T6, fwd).start()
        wait_in(qbuf, q_recv, at(T3, u, units))
        q_copy(4, u, T3, T4, fwd).start()
        q_copy(5, u, T3, T5, bwd).start()

    def relay2(u):
        wait_in(qbuf, q_recv, at(T6, u, units))
        q_copy(6, u, T6, T7, zp).start()

    def run_at(k, table):
        def choose(blocks):
            if len(blocks) == 1:

                @pl.when(k == blocks[0])
                def _():
                    for action in table[blocks[0]]:
                        action()

            else:
                middle = len(blocks) // 2
                lax.cond(
                    k < blocks[middle], lambda: choose(blocks[:middle]), lambda: choose(blocks[middle:])
                )

        choose(sorted(table))

    ahead_of = {}
    for block, u in ((1, 0), (2, 1), (3, 2), (4, 3)):
        ahead_of.setdefault(block, []).append(functools.partial(relay1, u))
    for block, u in ((4, 0), (5, 1), (6, 2), (7, 3)):
        ahead_of.setdefault(block, []).append(functools.partial(relay2, u))
    for n, (place, u) in enumerate(ORDER):
        if place in (T2, T5, T4, T7):
            ahead_of.setdefault((n - 1) // 2, []).append(functools.partial(wait_in, qbuf, q_recv, n))

    def leaf_out(place, u):
        number, slot, to = {T2: (0, IN02, fwd), T5: (1, IN35, fwd), T7: (2, IN67, zp), T4: (3, IN34, bwd)}[place]
        send_out(number, u, place, slot, to)

    def merge_out(place, u):
        number, slots, slot, to = {
            T6: (4, (IN67,), IN16, bwd),
            T3: (5, (IN34, IN35), IN03, zp),
            T1: (6, (IN16,), IN01, bwd),
        }[place]
        merge_send(number, u, place, slots, slot, to)

    def a_copy(number, u, place_from, place_to, to):
        k = place_to * units + u
        return remote(
            abuf.at[place_from * units + u], abuf.at[k], a_send.at[0], a_recv.at[k], to
        )

    def a_relay1(u):
        wait_in(abuf, a_recv, T3 * units + u)
        a_copy(5, u, T3, T5, bwd).start()
        if u >= units // 2:
            a_copy(1, u, T0, T2, bwd).start()
        wait_in(abuf, a_recv, T1 * units + u)
        a_copy(3, u, T1, T6, fwd).start()
        a_copy(4, u, T3, T4, fwd).start()

    def a_relay2(u):
        wait_in(abuf, a_recv, T6 * units + u)
        a_copy(6, u, T6, T7, zp).start()

    tile = tiles[me]
    limit = lengths[tile // 2 % 2, tile // 4] - tile % 2 * ROWS
    live = lax.broadcasted_iota(jnp.int32, (ROWS, UCOLS), 0) < limit
    def own_attention(u):
        o, _ = merged(u, T0, (IN02, IN03, IN01))
        abuf[T0 * units + u] = jnp.where(live, o, 0.0).astype(jnp.bfloat16)
        a_copy(0, u, T0, T1, fwd).start()
        if u < units // 2:
            a_copy(1, u, T0, T2, bwd).start()
        a_copy(2, u, T0, T3, zp).start()

    done_after = {
        block: [functools.partial(action, *args) for action, *args in actions]
        for block, actions in {
            2: [(leaf_out, T2, 0)],
            3: [(leaf_out, T2, 1)],
            5: [(leaf_out, T5, 0), (leaf_out, T5, 1)],
            6: [(leaf_out, T4, 0), (leaf_out, T4, 1)],
            7: [(leaf_out, T7, 0)],
            8: [(leaf_out, T7, 1)],
            9: [(leaf_out, T4, 2), (leaf_out, T4, 3), (merge_out, T6, 0)],
            10: [(leaf_out, T7, 2), (leaf_out, T7, 3), (merge_out, T6, 1), (merge_out, T3, 0)],
            11: [(merge_out, T1, 0), (merge_out, T3, 1)],
            12: [(merge_out, T1, 1), (leaf_out, T5, 2), (leaf_out, T5, 3), (merge_out, T6, 2), (merge_out, T6, 3)],
            13: [(own_attention, 0)],
            14: [(merge_out, T3, 2), (own_attention, 1)],
            15: [(leaf_out, T2, 2), (leaf_out, T2, 3), (merge_out, T3, 3), (merge_out, T1, 2), (merge_out, T1, 3)],
        }.items()
    }
    for block, actions in ahead_of.items():
        done_after.setdefault(block - 1, []).extend(actions)

    chunks = [(i * CHUNK, CHUNK) for i in range(2 * kd // CHUNK)]
    total_keys = 2 * kd

    def fold(op, x):
        parts = [x[:, i : i + 128] for i in range(0, x.shape[1], 128)]
        return functools.reduce(op, parts)

    def both(n1, s1, m1, n2, s2, m2, low2, sums2, acc2):
        first = n1 is not None
        second = n2 is not None
        if first:
            p1 = info[n1, 0]
            raw = qbuf[n1]
            query = jnp.concatenate([raw[:, i * WIDTH : (i + 1) * WIDTH] for i in range(HEADS_UNIT)], axis=0)
            peak = None
        if second:
            p2 = info[n2, 0]
            low = jnp.broadcast_to(jnp.max(m2[...], axis=1, keepdims=True) * SCALE, (UROWS, 128))
            sums = jnp.zeros((UROWS, 128), jnp.float32)
            acc = jnp.zeros((UROWS, WIDTH), jnp.float32)
        for at, size in chunks + [(total_keys, 2 * ROWS)]:
            own = at >= total_keys
            if first:
                keys = ckb[...] if own else kall[p1, pl.ds(at, size), :]
                s = across(query, keys)
                if own:
                    s = jnp.concatenate(
                        [
                            jnp.where(ahead <= info[n1, 1 + k], s[:, k * ROWS : (k + 1) * ROWS], VERY_LOW)
                            for k in range(2)
                        ],
                        axis=1,
                    )
                s1[:, pl.ds(at, size)] = s
                top = fold(jnp.maximum, s)
                peak = top if peak is None else jnp.maximum(peak, top)
            if second:
                rows = cvb[...] if own else vall[p2, pl.ds(at, size), :]
                w = jnp.exp2(s2[:, pl.ds(at, size)] * SCALE - jnp.concatenate([low] * (size // 128), axis=1))
                sums = sums + fold(jnp.add, w)
                acc = acc + jnp.dot(w.astype(jnp.bfloat16), rows, preferred_element_type=jnp.float32)
        if first:
            m1[...] = peak
        if second:
            low2[...] = low
            sums2[...] = sums
            acc2[...] = acc

    def finish(n, low2, sums2, acc2):
        total = jnp.sum(sums2[...], axis=1, keepdims=True)
        o = acc2[...] / total
        log = low2[...] + jnp.log2(total)
        for i in range(HEADS_UNIT):
            obuf[n, :, i * WIDTH : (i + 1) * WIDTH] = o[i * ROWS : (i + 1) * ROWS].astype(jnp.bfloat16)
            lob[n, i : i + 1, :] = log[i * ROWS : (i + 1) * ROWS].T[0:1, :]

    lob[...] = jnp.zeros_like(lob)
    sums_b[...] = jnp.ones_like(sums_b)
    for n in (0, 2, 4):
        loads[n].wait()
    kvs[0].wait_recv()
    kvs[1].wait_recv()
    both(0, sa, ma, None, None, None, None, None, None)
    for n in (1, 3) + tuple(range(5, 4 + units)):
        loads[n].wait()
    kvs[2].wait_recv()
    kvs[3].wait_recv()
    wload.start()
    wsend.start()

    def step(k, carry):
        n = 2 * k
        finish(jnp.maximum(n - 1, 0), low_b, sums_b, acc_b)
        both(n + 1, sb, mb, n, sa, ma, low_a, sums_a, acc_a)
        finish(n, low_a, sums_a, acc_a)
        both(jnp.minimum(n + 2, last), sa, ma, n + 1, sb, mb, low_b, sums_b, acc_b)
        run_at(k, done_after)
        return carry

    lax.fori_loop(0, 4 * units, step, 0)
    finish(last, low_b, sums_b, acc_b)

    a_relay1(0)
    a_relay1(1)
    own_attention(2)
    own_attention(3)

    f32 = jnp.float32
    half = ROWS // 2

    def piece_of(i):
        return (i + 2 * (1 - c)) % PIECES

    def x_copy(buf, sems, zt, piece, source, to):
        k = zt * PIECES + piece
        return remote(pbuf.at[source * PIECES + piece], buf.at[k], f_send.at[0], sems.at[k], to)

    def project(place):
        zf, steps = PLACES[place]
        home = seq(zf, steps) // 2
        rows = jnp.concatenate([abuf[place * units + u] for u in range(units)], axis=1)
        gap = (home // 2 - x + 4) % 4
        for part in range(2):
            r = jnp.dot(rows, wbuf[part], preferred_element_type=f32).astype(jnp.bfloat16)
            for i in range(2):
                pbuf[home * PIECES + part * 2 + i] = r[i * half : (i + 1) * half]
        for i in range(PIECES):
            piece = piece_of(i)

            @pl.when(gap == 2)
            def _():
                x_copy(far_in, far_recv, home % 2, piece, home, xbwd).start()

            @pl.when(gap == (d + 4) % 4)
            def _():
                x_copy(leaf_in, leaf_recv, home % 2, piece, home, xfwd).start()

    def settle(place):
        for u in range(units):
            wait_in(abuf, a_recv, place * units + u)

    def pass_on(place):
        zf, steps = PLACES[place]
        home = seq(zf, steps) // 2

        @pl.when((home // 2 - x + d + 4) % 4 == 0)
        def _():
            for i in range(PIECES):
                piece = piece_of(i)
                k, m = home % 2 * PIECES + piece, home * PIECES + piece
                wait_in(far_in, far_recv, k)
                pbuf[m] = (pbuf[m].astype(f32) + far_in[k].astype(f32)).astype(jnp.bfloat16)
                x_copy(inter_in, inter_recv, home % 2, piece, home, xbwd).start()

    wload.wait()
    wsend.wait_recv()
    project(T0)
    a_relay2(0)
    a_relay2(1)
    a_relay1(2)
    a_relay1(3)
    project(T3)
    project(T1)
    pass_on(T0)
    settle(T5)
    project(T5)
    settle(T2)
    project(T2)
    a_relay2(2)
    a_relay2(3)
    settle(T4)
    project(T4)
    project(T6)
    pass_on(T3)
    pass_on(T1)
    settle(T7)
    project(T7)
    pass_on(T5)
    pass_on(T2)
    pass_on(T4)
    pass_on(T6)
    pass_on(T7)

    def column_sum(zt, piece):
        k = zt * PIECES + piece
        wait_in(leaf_in, leaf_recv, k)
        wait_in(inter_in, inter_recv, k)
        here = pbuf[(x * 2 + zt) * PIECES + piece].astype(f32)
        return here + leaf_in[k].astype(f32) + inter_in[k].astype(f32)

    def z_copy(piece):
        return remote(zout.at[piece], zin.at[piece], f_send.at[0], z_recv.at[piece], zhp)

    for i in range(PIECES):
        piece = piece_of(i)
        zout[piece] = column_sum(1 - zh, piece).astype(jnp.bfloat16)
        z_copy(piece).start()
    for i in range(PIECES):
        piece = piece_of(i)
        fin[piece] = column_sum(zh, piece)
    last_copies = []
    for i in range(2):
        piece = (1 - c) * 2 + i
        wait_in(zin, z_recv, piece)
        xout[i] = (fin[piece] + zin[piece].astype(f32)).astype(jnp.bfloat16)
        rows = pl.ds(i * half, half)
        last_copies.append(remote(xout.at[i], out.at[c, rows], x_send.at[i], x_recv.at[i], other))
        last_copies[-1].start()
    for i in range(2):
        piece = c * 2 + i
        wait_in(zin, z_recv, piece)
        out[c, i * half : (i + 1) * half] = (fin[piece] + zin[piece].astype(f32)).astype(jnp.bfloat16)
    for copy in last_copies:
        copy.wait()

    for copy in kvs + [wsend]:
        copy.wait_send()
    for buf, sem in ((qbuf, q_send), (obuf, o_send), (lob, l_send), (abuf, a_send)):
        whole = buf.at[pl.ds(0, 7 * units)]
        pltpu.make_async_copy(whole, whole, sem.at[0]).wait()
    whole = pbuf.at[pl.ds(0, 7 * PIECES)]
    pltpu.make_async_copy(whole, whole, f_send.at[0]).wait()


def attend(lengths, prompts, tiles, q, ck, cv, pk, pv, weight):
    units = q.shape[2] // UCOLS
    assert units == UNITS
    kd = pk.shape[1]
    cols = weight.shape[1]
    keys = 2 * kd + 2 * ROWS
    bf, f32 = jnp.bfloat16, jnp.float32
    smem = pl.BlockSpec(memory_space=pltpu.SMEM)
    hbm = pl.BlockSpec(memory_space=pl.ANY)
    dma = pltpu.SemaphoreType.DMA
    return pl.pallas_call(
        functools.partial(attend_kernel, units),
        out_shape=jax.ShapeDtypeStruct((2, ROWS, weight.shape[1]), bf),
        in_specs=[smem] * 3 + [hbm] * 6,
        out_specs=pl.BlockSpec(memory_space=pltpu.VMEM),
        scratch_shapes=[
            pltpu.VMEM((2, 2 * kd, WIDTH), bf),
            pltpu.VMEM((2, 2 * kd, WIDTH), bf),
            pltpu.VMEM((2 * ROWS, WIDTH), bf),
            pltpu.VMEM((2 * ROWS, WIDTH), bf),
            pltpu.VMEM((8 * units, ROWS, UCOLS), bf),
            pltpu.VMEM((8 * units, ROWS, UCOLS), bf),
            pltpu.VMEM((7 * units, ROWS, UCOLS), bf),
            pltpu.VMEM((8 * units, 8, ROWS), f32),
            pltpu.VMEM((7 * units, 8, ROWS), f32),
            pltpu.VMEM((UROWS, keys), f32),
            pltpu.VMEM((UROWS, keys), f32),
            pltpu.VMEM((UROWS, 128), f32),
            pltpu.VMEM((UROWS, 128), f32),
            pltpu.VMEM((UROWS, 128), f32),
            pltpu.VMEM((UROWS, 128), f32),
            pltpu.VMEM((UROWS, 128), f32),
            pltpu.VMEM((UROWS, 128), f32),
            pltpu.VMEM((UROWS, 128), f32),
            pltpu.VMEM((UROWS, 128), f32),
            pltpu.SMEM((8 * units, 4), jnp.int32),
            pltpu.VMEM((2,) + weight.shape, bf),
            pltpu.VMEM((8 * units, ROWS, UCOLS), bf),
            pltpu.VMEM((8 * PIECES, ROWS // 2, cols), bf),
            pltpu.VMEM((2 * PIECES, ROWS // 2, cols), bf),
            pltpu.VMEM((2 * PIECES, ROWS // 2, cols), bf),
            pltpu.VMEM((2 * PIECES, ROWS // 2, cols), bf),
            pltpu.VMEM((PIECES, ROWS // 2, cols), bf),
            pltpu.VMEM((PIECES, ROWS // 2, cols), bf),
            pltpu.VMEM((PIECES, ROWS // 2, cols), f32),
            pltpu.VMEM((2, ROWS // 2, cols), bf),
            dma((5 + units,)),
            dma((5,)),
            dma((5,)),
            dma((1,)),
            dma((8 * units,)),
            dma((1,)),
            dma((7 * units,)),
            dma((1,)),
            dma((1,)),
            dma((8 * units,)),
            dma((2 * PIECES,)),
            dma((2 * PIECES,)),
            dma((2 * PIECES,)),
            dma((PIECES,)),
            dma((1,)),
            dma((2,)),
            dma((2,)),
        ],
        compiler_params=pltpu.CompilerParams(
            collective_id=0, has_side_effects=True, vmem_limit_bytes=60 << 20
        ),
        name="attend",
    )(lengths, prompts, tiles, q, ck, cv, pk, pv, weight)


def local(q, ck, cv, pk, pv, lengths, prompts, tiles, weight):
    return attend(lengths.T, prompts, tiles, q, ck, cv, pk, pv, weight)


def solution(mesh):
    return jax.shard_map(
        local,
        mesh=mesh,
        in_specs=(
            P("seq", None, "head"),
            P("seq", None, "head"),
            P("seq", None, "head"),
            P(None, "seq", "head"),
            P(None, "seq", "head"),
            P(),
            P(),
            P(),
            P("head", "seq"),
        ),
        out_specs=P("head", None, "seq"),
        check_vma=False,
    )
```
